8 devices in a mesh: dp: 1 (over z), tp: 8 (over y, x, core).
Axes of the slice: x: 2, y: 2, z: 1, core: 2. Of those that a mesh axis runs over, the one named last changes fastest.
Arguments:
- tokens: bfloat16 [3, 1024, 4096], P('dp', 'tp')
- start_pos: int32 [3], P('dp')
- cos_tab: float32 [3, 1024, 128], P('dp')
- sin_tab: float32 [3, 1024, 128], P('dp')
- key_cache: bfloat16 [2, 3, 4096, 8, 128], P(None, 'dp', None, 'tp')
- value_cache: bfloat16 [2, 3, 4096, 8, 128], P(None, 'dp', None, 'tp')
- slot_pos: int32 [3, 4096], P('dp')
- norm_params: bfloat16 [2, 4, 4096], replicated
- w_q: bfloat16 [2, 4096, 4096], P(None, None, 'tp')
- b_q: bfloat16 [2, 4096], P(None, 'tp')
- w_k: bfloat16 [2, 4096, 1024], P(None, None, 'tp')
- b_k: bfloat16 [2, 1024], P(None, 'tp')
- w_v: bfloat16 [2, 4096, 1024], P(None, None, 'tp')
- b_v: bfloat16 [2, 1024], P(None, 'tp')
- w_o: bfloat16 [2, 4096, 4096], P(None, 'tp')
- b_o: bfloat16 [2, 4096], replicated
- w_up: bfloat16 [2, 4096, 14336], P(None, None, 'tp')
- b_up: bfloat16 [2, 14336], P(None, 'tp')
- w_down: bfloat16 [2, 14336, 4096], P(None, 'tp')
- b_down: bfloat16 [2, 4096], replicated
Outputs:
- output 1: bfloat16 [3, 1024, 4096], P('dp', 'tp')
- output 2: bfloat16 [2, 3, 4096, 8, 128], P(None, 'dp', None, 'tp')
- output 3: bfloat16 [2, 3, 4096, 8, 128], P(None, 'dp', None, 'tp')
- output 4: int32 [3, 4096], P('dp')
All inputs are finite; a program needn't handle non-finite values.
Results may differ from the reference program's by a relative error of at most 0.02.
Values are sent between devices in bfloat16 or wider.
A program may use at most 1 GiB of HBM per device.

```python
import jax
import jax.numpy as jnp
from jax import lax

NUM_SEQS = 3
CHUNK_LEN = 1024
MODEL_DIM = 4096
NUM_HEADS = 32
KV_HEADS = 8
HEAD_DIM = 128
FFN_DIM = 14336
WINDOW = 4096
NUM_LAYERS = 2
NORM_EPS = 1e-5
ROPE_BASE = 1000000.0


def draw_positions(start_key):
    drawn = jax.random.randint(start_key, (NUM_SEQS,), 0, 3 * WINDOW)
    start_pos = jnp.where(jnp.arange(NUM_SEQS) == 0, drawn % WINDOW, drawn).astype(jnp.int32)
    slots = jnp.arange(WINDOW)
    latest = start_pos[:, None] - 1 - (start_pos[:, None] - 1 - slots[None, :]) % WINDOW
    slot_pos = jnp.where(latest >= 0, latest, -1).astype(jnp.int32)
    return start_pos, slot_pos


def rotary_tables(start_pos):
    positions = (start_pos[:, None] + jnp.arange(CHUNK_LEN)[None, :]).astype(jnp.float32)
    inv_freq = ROPE_BASE ** (-jnp.arange(0, HEAD_DIM, 2).astype(jnp.float32) / HEAD_DIM)
    angles = positions[:, :, None] * inv_freq[None, None, :]
    angles = jnp.concatenate([angles, angles], axis=-1)
    return jnp.cos(angles), jnp.sin(angles)


def normal_draw(key, shape, scale):
    return (jax.random.normal(key, shape, jnp.float32) * scale).astype(jnp.bfloat16)


def setup_inputs(seed: int = 0, part: int = 0) -> dict:
    part_keys = jax.random.split(jax.random.fold_in(jax.random.key(seed), part), 4)
    weight_keys = jax.random.split(jax.random.key(seed + 1), 13)
    start_pos, slot_pos = draw_positions(part_keys[1])
    cos_tab, sin_tab = rotary_tables(start_pos)
    cache_shape = (NUM_LAYERS, NUM_SEQS, WINDOW, KV_HEADS, HEAD_DIM)
    q_width = NUM_HEADS * HEAD_DIM
    kv_width = KV_HEADS * HEAD_DIM
    norm_base = jnp.array([1.0, 0.0, 1.0, 0.0], jnp.float32)[None, :, None]
    norm_spread = jnp.array([0.25, 0.2, 0.25, 0.2], jnp.float32)[None, :, None]
    norm_noise = jax.random.normal(weight_keys[0], (NUM_LAYERS, 4, MODEL_DIM), jnp.float32)
    return {
        'tokens': normal_draw(part_keys[0], (NUM_SEQS, CHUNK_LEN, MODEL_DIM), 1.0),
        'start_pos': start_pos,
        'cos_tab': cos_tab,
        'sin_tab': sin_tab,
        'key_cache': normal_draw(part_keys[2], cache_shape, 1.0),
        'value_cache': normal_draw(part_keys[3], cache_shape, 1.0),
        'slot_pos': slot_pos,
        'norm_params': (norm_base + norm_spread * norm_noise).astype(jnp.bfloat16),
        'w_q': normal_draw(weight_keys[1], (NUM_LAYERS, MODEL_DIM, q_width), 2.5 * MODEL_DIM ** -0.5),
        'b_q': normal_draw(weight_keys[2], (NUM_LAYERS, q_width), 0.5),
        'w_k': normal_draw(weight_keys[3], (NUM_LAYERS, MODEL_DIM, kv_width), MODEL_DIM ** -0.5),
        'b_k': normal_draw(weight_keys[4], (NUM_LAYERS, kv_width), 0.5),
        'w_v': normal_draw(weight_keys[5], (NUM_LAYERS, MODEL_DIM, kv_width), MODEL_DIM ** -0.5),
        'b_v': normal_draw(weight_keys[6], (NUM_LAYERS, kv_width), 0.5),
        'w_o': normal_draw(weight_keys[7], (NUM_LAYERS, q_width, MODEL_DIM), 2.0 * q_width ** -0.5),
        'b_o': normal_draw(weight_keys[8], (NUM_LAYERS, MODEL_DIM), 0.3),
        'w_up': normal_draw(weight_keys[9], (NUM_LAYERS, MODEL_DIM, FFN_DIM), MODEL_DIM ** -0.5),
        'b_up': normal_draw(weight_keys[10], (NUM_LAYERS, FFN_DIM), 0.5),
        'w_down': normal_draw(weight_keys[11], (NUM_LAYERS, FFN_DIM, MODEL_DIM), FFN_DIM ** -0.5),
        'b_down': normal_draw(weight_keys[12], (NUM_LAYERS, MODEL_DIM), 0.3),
    }


def layer_norm(hidden, gain, shift):
    values = hidden.astype(jnp.float32)
    centered = values - jnp.mean(values, axis=-1, keepdims=True)
    variance = jnp.mean(centered * centered, axis=-1, keepdims=True)
    scaled = centered * lax.rsqrt(variance + NORM_EPS)
    return (scaled * gain.astype(jnp.float32) + shift.astype(jnp.float32)).astype(jnp.bfloat16)


def apply_rotary(values, cos_b, sin_b):
    half = values.shape[-1] // 2
    turned = jnp.concatenate([-values[..., half:], values[..., :half]], axis=-1)
    return (values * cos_b + turned * sin_b).astype(jnp.bfloat16)


def attend_group(group_in, old_ok, new_ok):
    query, key_new, value_new, cache_k, cache_v = group_in
    scale = HEAD_DIM ** -0.5
    score_old = jnp.einsum('gcd,wd->gcw', query.astype(jnp.float32), cache_k.astype(jnp.float32)) * scale
    score_new = jnp.einsum('gcd,jd->gcj', query.astype(jnp.float32), key_new.astype(jnp.float32)) * scale
    score_old = jnp.where(old_ok[None], score_old, -jnp.inf)
    score_new = jnp.where(new_ok[None], score_new, -jnp.inf)
    top = jnp.maximum(jnp.max(score_old, axis=-1, keepdims=True), jnp.max(score_new, axis=-1, keepdims=True))
    exp_old = jnp.exp(score_old - top)
    exp_new = jnp.exp(score_new - top)
    total = jnp.sum(exp_old, axis=-1, keepdims=True) + jnp.sum(exp_new, axis=-1, keepdims=True)
    mixed = jnp.einsum('gcw,wd->gcd', exp_old.astype(jnp.bfloat16).astype(jnp.float32), cache_v.astype(jnp.float32))
    mixed = mixed + jnp.einsum('gcj,jd->gcd', exp_new.astype(jnp.bfloat16).astype(jnp.float32), value_new.astype(jnp.float32))
    return (mixed / total).astype(jnp.bfloat16)


def attend_sequence(seq_inputs):
    query, key_new, value_new, cache_k, cache_v, held_pos, first_pos = seq_inputs
    positions = first_pos + jnp.arange(CHUNK_LEN)
    old_ok = (held_pos[None, :] >= 0) & (held_pos[None, :] > positions[:, None] - WINDOW) & (held_pos[None, :] <= positions[:, None])
    new_ok = jnp.arange(CHUNK_LEN)[None, :] <= jnp.arange(CHUNK_LEN)[:, None]
    grouped = query.reshape(CHUNK_LEN, KV_HEADS, NUM_HEADS // KV_HEADS, HEAD_DIM).transpose(1, 2, 0, 3)
    per_group = lax.map(lambda group_in: attend_group(group_in, old_ok, new_ok), (grouped, key_new.transpose(1, 0, 2), value_new.transpose(1, 0, 2), cache_k.transpose(1, 0, 2), cache_v.transpose(1, 0, 2)))
    return per_group.transpose(2, 0, 1, 3).reshape(CHUNK_LEN, NUM_HEADS * HEAD_DIM)


def reference(tokens, start_pos, cos_tab, sin_tab, key_cache, value_cache, slot_pos, norm_params, w_q, b_q, w_k, b_k, w_v, b_v, w_o, b_o, w_up, b_up, w_down, b_down):
    positions = start_pos[:, None] + jnp.arange(CHUNK_LEN)[None, :]
    slots = positions % WINDOW
    rows = jnp.arange(NUM_SEQS)[:, None]
    cos_b = cos_tab[:, :, None, :]
    sin_b = sin_tab[:, :, None, :]
    tok_count = NUM_SEQS * CHUNK_LEN

    def layer_step(hidden, layer_in):
        cache_k, cache_v, norms, proj_q, bias_q, proj_k, bias_k, proj_v, bias_v, proj_o, bias_o, proj_up, bias_up, proj_down, bias_down = layer_in
        normed = layer_norm(hidden, norms[0], norms[1]).reshape(tok_count, MODEL_DIM)
        query = jnp.dot(normed, proj_q, preferred_element_type=jnp.float32) + bias_q.astype(jnp.float32)
        query = apply_rotary(query.reshape(NUM_SEQS, CHUNK_LEN, NUM_HEADS, HEAD_DIM), cos_b, sin_b)
        key_new = jnp.dot(normed, proj_k, preferred_element_type=jnp.float32) + bias_k.astype(jnp.float32)
        key_new = apply_rotary(key_new.reshape(NUM_SEQS, CHUNK_LEN, KV_HEADS, HEAD_DIM), cos_b, sin_b)
        value_new = (jnp.dot(normed, proj_v, preferred_element_type=jnp.float32) + bias_v.astype(jnp.float32)).astype(jnp.bfloat16)
        value_new = value_new.reshape(NUM_SEQS, CHUNK_LEN, KV_HEADS, HEAD_DIM)
        mixed = lax.map(attend_sequence, (query, key_new, value_new, cache_k, cache_v, slot_pos, start_pos))
        attended = jnp.dot(mixed.reshape(tok_count, NUM_HEADS * HEAD_DIM), proj_o, preferred_element_type=jnp.float32)
        middle = (hidden.astype(jnp.float32) + attended.reshape(NUM_SEQS, CHUNK_LEN, MODEL_DIM) + bias_o.astype(jnp.float32)).astype(jnp.bfloat16)
        normed = layer_norm(middle, norms[2], norms[3]).reshape(tok_count, MODEL_DIM)
        lifted = jnp.dot(normed, proj_up, preferred_element_type=jnp.float32) + bias_up.astype(jnp.float32)
        active = jax.nn.gelu(lifted, approximate=True).astype(jnp.bfloat16)
        lowered = jnp.dot(active, proj_down, preferred_element_type=jnp.float32).reshape(NUM_SEQS, CHUNK_LEN, MODEL_DIM)
        layer_out = (middle.astype(jnp.float32) + lowered + bias_down.astype(jnp.float32)).astype(jnp.bfloat16)
        new_k = cache_k.at[rows, slots].set(key_new)
        new_v = cache_v.at[rows, slots].set(value_new)
        return layer_out, (new_k, new_v)

    final, (key_out, value_out) = lax.scan(layer_step, tokens, (key_cache, value_cache, norm_params, w_q, b_q, w_k, b_k, w_v, b_v, w_o, b_o, w_up, b_up, w_down, b_down))
    pos_out = slot_pos.at[rows, slots].set(positions.astype(jnp.int32))
    return final, key_out, value_out, pos_out
```

```python
import functools

import jax
import jax.numpy as jnp
from jax import lax
from jax.experimental import pallas as pl
from jax.experimental.pallas import tpu as pltpu
from jax.sharding import PartitionSpec as P


NORM_EPS = 1e-5
LOG2E = 1.4426950408889634
HIDE = -(1 << 30)
TURNS = [int(c) for c in '012010120201120210120021120210120101220210120210122']


def norm_kernel(*refs, joined):
    if joined:
        base_ref, pair_ref, came_ref, last_ref, bias_ref, gain_ref, shift_ref, sum_ref, norm_ref = refs
        summed = pair_ref[...].astype(jnp.float32) + came_ref[...].astype(jnp.float32) + last_ref[...].astype(jnp.float32)
        kept = (base_ref[...].astype(jnp.float32) + summed + bias_ref[...].astype(jnp.float32)).astype(jnp.bfloat16)
        sum_ref[...] = kept
    else:
        base_ref, gain_ref, shift_ref, norm_ref = refs
        kept = base_ref[...]
    values = kept.astype(jnp.float32)
    centered = values - jnp.mean(values, axis=-1, keepdims=True)
    variance = jnp.mean(centered * centered, axis=-1, keepdims=True)
    scaled = centered * lax.rsqrt(variance + NORM_EPS)
    norm_ref[...] = (scaled * gain_ref[...].astype(jnp.float32) + shift_ref[...].astype(jnp.float32)).astype(jnp.bfloat16)


def normalize(base, seq, terms, bias, norms, layer, which, rows=32):
    part, model = base.shape[-2:]
    line = pl.BlockSpec((rows, model), lambda i: (i, 0))
    first = line if base.ndim == 2 else pl.BlockSpec((None, rows, model), lambda i: (seq, i, 0))
    vector = lambda at: pl.BlockSpec((None, 1, model), lambda i: (at, 0, 0))
    scale_specs = [vector(4 * layer + which), vector(4 * layer + which + 1)]
    scales = [norms, norms]
    whole = jax.ShapeDtypeStruct((part, model), jnp.bfloat16)
    if terms is None:
        specs, args, outs = [first], [base], [whole]
    else:
        bias, bias_at = bias
        specs, args, outs = [first, line, line, line, vector(bias_at)], [base, *terms, bias], [whole, whole]
    return pl.pallas_call(
        functools.partial(norm_kernel, joined=terms is not None),
        grid=(part // rows,),
        in_specs=specs + scale_specs,
        out_specs=[line] * len(outs),
        out_shape=outs,
        compiler_params=pltpu.CompilerParams(dimension_semantics=('arbitrary',), vmem_limit_bytes=16 << 20),
        cost_estimate=pl.CostEstimate(flops=8 * part * model, bytes_accessed=2 * (len(args) + len(outs)) * part * model, transcendentals=0),
        name='norm',
    )(*args, *scales)


def qkv_kernel(x_ref, cos_ref, sin_ref, wq_ref, wk_ref, wv_ref, bq_ref, bk_ref, bv_ref, q_ref, k_ref, v_ref):
    head_dim = cos_ref.shape[-1]
    acts = x_ref[...]
    cos_b = cos_ref[...]
    lane = lax.broadcasted_iota(jnp.int32, cos_b.shape, 1)
    sin_b = jnp.where(lane < head_dim // 2, -sin_ref[...], sin_ref[...])

    def rotary(values):
        return (values * cos_b + pltpu.roll(values, head_dim // 2, 1) * sin_b).astype(jnp.bfloat16)

    query = jnp.dot(acts, wq_ref[...], preferred_element_type=jnp.float32) + bq_ref[...].astype(jnp.float32)
    for head in range(query.shape[1] // head_dim):
        cols = slice(head * head_dim, (head + 1) * head_dim)
        q_ref[:, cols] = rotary(query[:, cols])
    weight_kv = jnp.concatenate([wk_ref[...], wv_ref[...]], axis=1)
    key_value = jnp.dot(acts, weight_kv, preferred_element_type=jnp.float32)
    k_ref[...] = rotary(key_value[:, :head_dim] + bk_ref[...].astype(jnp.float32))
    v_ref[...] = (key_value[:, head_dim:] + bv_ref[...].astype(jnp.float32)).astype(jnp.bfloat16)


def qkv_project(acts, cos_tab, sin_tab, w_q, w_k, w_v, b_q, b_k, b_v, layer, seq, rows=256):
    chunk, model = acts.shape
    head_dim = cos_tab.shape[-1]
    q_cols = w_q.shape[2]
    kv_cols = w_k.shape[2]
    row_block = lambda cols: pl.BlockSpec((rows, cols), lambda i: (i, 0))
    table = pl.BlockSpec((None, rows, head_dim), lambda i: (seq, i, 0))
    weight = lambda cols: pl.BlockSpec((None, model, cols), lambda i: (layer, 0, 0))
    bias = lambda cols: pl.BlockSpec((None, 1, cols), lambda i: (layer, 0, 0))
    return pl.pallas_call(
        qkv_kernel,
        grid=(chunk // rows,),
        in_specs=[row_block(model), table, table, weight(q_cols), weight(kv_cols), weight(kv_cols), bias(q_cols), bias(kv_cols), bias(kv_cols)],
        out_specs=[row_block(q_cols), row_block(kv_cols), row_block(kv_cols)],
        out_shape=[jax.ShapeDtypeStruct((chunk, cols), jnp.bfloat16) for cols in (q_cols, kv_cols, kv_cols)],
        compiler_params=pltpu.CompilerParams(dimension_semantics=('arbitrary',), vmem_limit_bytes=40 << 20),
        cost_estimate=pl.CostEstimate(flops=2 * chunk * model * (q_cols + 2 * kv_cols), bytes_accessed=2 * (chunk + q_cols + 2 * kv_cols) * model, transcendentals=0),
        name='qkv_rotary',
    )(acts, cos_tab, sin_tab, w_q, w_k, w_v, b_q[:, None, :], b_k[:, None, :], b_v[:, None, :])


def attention_kernel(place_ref, start_ref, q_ref, kn_ref, vn_ref, ko_ref, vo_ref, held_ref, o_ref, score_ref, *, seq, group, key_block):
    rows = q_ref.shape[0]
    head_dim = kn_ref.shape[1]
    window = ko_ref.shape[0]
    block = pl.program_id(0)
    start = start_ref[seq]
    scale = head_dim ** -0.5 * LOG2E
    query = jnp.concatenate([q_ref[:, g * head_dim:(g + 1) * head_dim] for g in range(group)], axis=0)
    token = block * rows + lax.broadcasted_iota(jnp.int32, (rows, 1), 0)
    token = jnp.concatenate([token] * group, axis=0)
    oldest = start + token - window
    top_shape = (rows * group, 128)

    def lane_max(values, top):
        for i in range(values.shape[1] // 128):
            top = jnp.maximum(top, values[:, i * 128:(i + 1) * 128])
        return top

    def lane_sum(values, total):
        for i in range(values.shape[1] // 128):
            total = total + values[:, i * 128:(i + 1) * 128]
        return total

    contract = (((1,), (1,)), ((), ()))

    def score_old(step, top):
        at = pl.multiple_of(step * key_block, key_block)
        values = lax.dot_general(query, ko_ref[pl.ds(at, key_block), :], contract, preferred_element_type=jnp.float32)
        held = held_ref[:, pl.ds(at, key_block)]
        held = jnp.where((held >= 0) & (held < start), held, HIDE)
        values = jnp.where(held > oldest, values, -jnp.inf)
        score_ref[:, pl.ds(at, key_block)] = values
        return lane_max(values, top)

    def score_new(step, top):
        at = pl.multiple_of(step * key_block, key_block)
        values = lax.dot_general(query, kn_ref[pl.ds(at, key_block), :], contract, preferred_element_type=jnp.float32)
        fresh = at + lax.broadcasted_iota(jnp.int32, (1, key_block), 1)
        values = jnp.where(fresh <= token, values, -jnp.inf)
        score_ref[:, pl.ds(pl.multiple_of(window + at, key_block), key_block)] = values
        return lane_max(values, top)

    new_steps = (block * rows + rows + key_block - 1) // key_block
    top = jnp.full(top_shape, -jnp.inf, jnp.float32)
    top = lax.fori_loop(0, window // key_block, score_old, top)
    top = lax.fori_loop(0, new_steps, score_new, top)
    top = jnp.max(top, axis=1, keepdims=True)

    def weigh(at, value_ref, value_at, carry):
        total, mixed = carry
        weights = jnp.exp2((score_ref[:, pl.ds(at, key_block)] - top) * scale)
        total = lane_sum(weights, total)
        mixed = mixed + jnp.dot(weights.astype(jnp.bfloat16), value_ref[pl.ds(value_at, key_block), :], preferred_element_type=jnp.float32)
        return total, mixed

    def mix_old(step, carry):
        at = pl.multiple_of(step * key_block, key_block)
        return weigh(at, vo_ref, at, carry)

    def mix_new(step, carry):
        at = pl.multiple_of(step * key_block, key_block)
        return weigh(pl.multiple_of(window + at, key_block), vn_ref, at, carry)

    carry = (jnp.zeros(top_shape, jnp.float32), jnp.zeros((rows * group, head_dim), jnp.float32))
    carry = lax.fori_loop(0, window // key_block, mix_old, carry)
    total, mixed = lax.fori_loop(0, new_steps, mix_new, carry)
    mixed = (mixed / jnp.sum(total, axis=1, keepdims=True)).astype(jnp.bfloat16)
    for g in range(group):
        o_ref[:, g * head_dim:(g + 1) * head_dim] = mixed[g * rows:(g + 1) * rows]


def attend(query, key_new, value_new, key_cache, value_cache, held, place, start_pos, layer, seq, rows=128, key_block=512):
    chunk, q_cols = query.shape
    window, head_dim = key_cache.shape[2:]
    group = q_cols // head_dim
    keys = window + chunk
    whole = pl.BlockSpec((chunk, head_dim), lambda i, *_: (0, 0))
    cache = pl.BlockSpec((None, None, window, head_dim), lambda i, *_: (layer, seq, 0, 0))
    return pl.pallas_call(
        functools.partial(attention_kernel, seq=seq, group=group, key_block=key_block),
        grid_spec=pltpu.PrefetchScalarGridSpec(
            num_scalar_prefetch=2,
            grid=(chunk // rows,),
            in_specs=[pl.BlockSpec((rows, q_cols), lambda i, *_: (i, 0)), whole, whole, cache, cache, pl.BlockSpec((None, 1, window), lambda i, *_: (seq, 0, 0))],
            out_specs=pl.BlockSpec((rows, q_cols), lambda i, place, start: (place[i], 0)),
            scratch_shapes=[pltpu.VMEM((rows * group, keys), jnp.float32)],
        ),
        out_shape=jax.ShapeDtypeStruct((chunk, q_cols), jnp.bfloat16),
        compiler_params=pltpu.CompilerParams(dimension_semantics=('arbitrary',), vmem_limit_bytes=40 << 20),
        cost_estimate=pl.CostEstimate(flops=8 * chunk * q_cols * keys, bytes_accessed=4 * (window + chunk) * head_dim + 4 * chunk * q_cols, transcendentals=0),
        name='attend',
    )(place, start_pos, query, key_new, value_new, key_cache, value_cache, held)


def cache_kernel(start_ref, ko_ref, vo_ref, kn_ref, vn_ref, kout_ref, vout_ref, ring_ref):
    window, head_dim = ko_ref.shape
    chunk = kn_ref.shape[0]
    pad = 16
    span = chunk + pad
    first = lax.rem(start_ref[pl.program_id(1)], window)
    base = pl.multiple_of((first // pad) * pad, pad)
    inner = first - base
    line = lax.broadcasted_iota(jnp.int32, (span, head_dim), 0)
    for old_ref, new_ref, out_ref in ((ko_ref, kn_ref, kout_ref), (vo_ref, vn_ref, vout_ref)):
        ring_ref[0:window] = old_ref[...]
        ring_ref[window:window + span] = old_ref[0:span]
        fresh = jnp.concatenate([new_ref[...].astype(jnp.float32), jnp.zeros((pad, head_dim), jnp.float32)], axis=0)
        fresh = pltpu.roll(fresh, inner, 0)
        kept = ring_ref[pl.ds(base, span), :].astype(jnp.float32)
        mine = (line >= inner) & (line < inner + chunk)
        ring_ref[pl.ds(base, span), :] = jnp.where(mine, fresh, kept).astype(jnp.bfloat16)
        out_ref[span:window] = ring_ref[span:window]
        wrapped = ring_ref[window:window + span].astype(jnp.float32)
        plain = ring_ref[0:span].astype(jnp.float32)
        out_ref[0:span] = jnp.where(line < first + chunk - window, wrapped, plain).astype(jnp.bfloat16)


def update_caches(start_pos, key_cache, value_cache, key_new, value_new):
    layers, seqs, window, head_dim = key_cache.shape
    chunk = key_new.shape[2]
    old = pl.BlockSpec((None, None, window, head_dim), lambda i, j, *_: (i, j, 0, 0))
    new = pl.BlockSpec((None, None, chunk, head_dim), lambda i, j, *_: (i, j, 0, 0))
    return pl.pallas_call(
        cache_kernel,
        grid_spec=pltpu.PrefetchScalarGridSpec(
            num_scalar_prefetch=1,
            grid=(layers, seqs),
            in_specs=[old, old, new, new],
            out_specs=[old, old],
            scratch_shapes=[pltpu.VMEM((window + chunk + 16, head_dim), jnp.bfloat16)],
        ),
        out_shape=[jax.ShapeDtypeStruct(key_cache.shape, jnp.bfloat16)] * 2,
        compiler_params=pltpu.CompilerParams(dimension_semantics=('arbitrary', 'arbitrary'), vmem_limit_bytes=32 << 20),
        cost_estimate=pl.CostEstimate(flops=1 << 24, bytes_accessed=8 * layers * seqs * window * head_dim, transcendentals=0),
        name='write_caches',
    )(start_pos, key_cache, value_cache, key_new, value_new)


def solution(mesh):
    row_spec = P('dp', 'tp', None)
    cache_spec = P(None, 'dp', None, 'tp', None)
    col_spec = P(None, None, 'tp')
    bias_spec = P(None, 'tp')
    in_specs = (row_spec, P('dp'), P('dp', None, None), P('dp', None, None), cache_spec, cache_spec, P('dp', None), P(), col_spec, bias_spec, col_spec, bias_spec, col_spec, bias_spec, P(None, 'tp', None), P(), col_spec, bias_spec, P(None, 'tp', None), P())
    out_specs = (row_spec, cache_spec, cache_spec, P('dp', None))
    count = mesh.shape['tp']
    first_axis = lambda core: 1 + core
    pairs_core = [(d, d ^ 1) for d in range(count)]
    pairs_first = [(d, ((d // 2) ^ first_axis(d % 2)) * 2 + d % 2) for d in range(count)]
    pairs_second = [(d, ((d // 2) ^ (3 - first_axis(d % 2))) * 2 + d % 2) for d in range(count)]

    def device_step(tokens, start_pos, cos_tab, sin_tab, key_cache, value_cache, slot_pos, norm_params, w_q, b_q, w_k, b_k, w_v, b_v, w_o, b_o, w_up, b_up, w_down, b_down):
        num_seqs, part, model = tokens.shape
        chunk = cos_tab.shape[1]
        head_dim = cos_tab.shape[2]
        layers = key_cache.shape[0]
        window = key_cache.shape[2]
        keys_in = key_cache.reshape(layers, num_seqs, window, head_dim)
        values_in = value_cache.reshape(layers, num_seqs, window, head_dim)
        held = slot_pos[:, None, :]
        me = lax.axis_index('tp')
        chip, core = me // 2, me % 2
        near, far = 1 + core, 2 - core
        mine = [chip ^ flip for flip in (0, far, near, 3)]
        theirs = [chip ^ flip for flip in (0, near, far, 3)]
        order = [c * 2 + core for c in mine] + [c * 2 + 1 - core for c in theirs]
        table = jnp.stack(order).astype(jnp.int32)
        place = jnp.sum(jnp.where(table[None, :] == jnp.arange(count)[:, None], jnp.arange(count)[None, :], 0), axis=1).astype(jnp.int32)
        half = chunk // 2

        norms = norm_params.reshape(-1, 1, model)
        out_bias = b_o[:, None, :]
        down_bias = b_down[:, None, :]
        latest = [None]
        turn = [0]

        def item(compute, *values):
            if latest[0] is not None:
                values = lax.optimization_barrier((*values, latest[0]))[:-1]
            results = compute(*values)
            latest[0] = results[0]
            return results

        def send(value, pairs):
            return lax.ppermute(value, 'tp', pairs)

        def gather(value):
            return lax.all_gather(value, 'tp', axis=0, tiled=True)

        def add_lead(own, lead, weight):
            return ((jnp.dot(own, weight, preferred_element_type=jnp.float32) + lead.astype(jnp.float32)).astype(jnp.bfloat16),)

        def add_came(pair, came):
            return ((pair[part:2 * part].astype(jnp.float32) + came[part:].astype(jnp.float32)).astype(jnp.bfloat16),)

        def scatter_sum(lead, own, weight):
            lead = send(lead, pairs_core)
            yield
            pair, = item(functools.partial(add_lead, weight=weight), own, lead)
            came = send(pair[2 * part:], pairs_first)
            yield
            onward, = item(add_came, pair, came)
            last = send(onward, pairs_second)
            yield
            return pair, came, last

        def attention(gathered, layer, seq):
            query, key_new, value_new = qkv_project(gathered, cos_tab, sin_tab, w_q, w_k, w_v, b_q, b_k, b_v, layer, seq)
            fresh_keys[layer][seq] = key_new
            fresh_values[layer][seq] = value_new
            mixed = attend(query, key_new, value_new, keys_in, values_in, held, place, start_pos, layer, seq)
            lead = jnp.dot(mixed[half:], w_o[layer], preferred_element_type=jnp.float32).astype(jnp.bfloat16)
            return lead, mixed[:half]

        def expand(gathered, layer):
            lifted = jnp.dot(gathered, w_up[layer], preferred_element_type=jnp.float32) + b_up[layer].astype(jnp.float32)
            active = jax.nn.gelu(lifted, approximate=True).astype(jnp.bfloat16)
            pick = lambda indices: jnp.concatenate([lax.dynamic_slice_in_dim(active, index * part, part, 0) for index in indices], axis=0)
            lead = jnp.dot(pick(order[4:]), w_down[layer], preferred_element_type=jnp.float32).astype(jnp.bfloat16)
            return lead, pick(order[:4])

        def finish(middle, pair, came, last):
            summed = pair[:part].astype(jnp.float32) + came[:part].astype(jnp.float32) + last.astype(jnp.float32)
            return ((middle.astype(jnp.float32) + summed + b_down[layers - 1].astype(jnp.float32)).astype(jnp.bfloat16),)

        def join(base, *terms, bias, layer, which):
            middle, normed = normalize(base, seq_of[0], terms, (bias, layer), norms, layer + which // 4, which % 4)
            return normed, middle

        seq_of = [0]
        fresh_keys = [[None] * num_seqs for _ in range(layers)]
        fresh_values = [[None] * num_seqs for _ in range(layers)]
        hidden_out = [None] * num_seqs

        def stream(seq):
            base = tokens
            normed, = item(lambda: normalize(base, seq, None, None, norms, 0, 0))
            for layer in range(layers):
                gathered = gather(normed)
                yield
                lead, own = item(functools.partial(attention, layer=layer, seq=seq), gathered)
                terms = yield from scatter_sum(lead, own, w_o[layer])
                seq_of[0] = seq
                normed, middle = item(lambda *terms: join(base, *terms, bias=out_bias, layer=layer, which=2), *terms)
                gathered = gather(normed)
                yield
                lead, own = item(functools.partial(expand, layer=layer), gathered)
                terms = yield from scatter_sum(lead, own, w_down[layer])
                if layer + 1 < layers:
                    seq_of[0] = seq
                    normed, base = item(lambda *terms: join(middle, *terms, bias=down_bias, layer=layer, which=4), *terms)
                else:
                    hidden_out[seq], = item(finish, middle, *terms)
            yield

        streams = [stream(seq) for seq in range(num_seqs)]
        for step, seq in enumerate(TURNS):
            turn[0] = step
            next(streams[seq])
        fresh_keys = [jnp.stack(k) for k in fresh_keys]
        fresh_values = [jnp.stack(v) for v in fresh_values]
        key_out, value_out = update_caches(start_pos, keys_in, values_in, jnp.stack(fresh_keys), jnp.stack(fresh_values))
        first_slot = start_pos % window
        offset = (jnp.arange(window)[None, :] - first_slot[:, None]) % window
        pos_out = jnp.where(offset < chunk, start_pos[:, None] + offset, slot_pos)
        return jnp.stack(hidden_out), key_out.reshape(key_cache.shape), value_out.reshape(value_cache.shape), pos_out

    return jax.shard_map(device_step, mesh=mesh, in_specs=in_specs, out_specs=out_specs, check_vma=False)
```

```python
import functools

import jax
import jax.numpy as jnp
from jax import lax
from jax.experimental import pallas as pl
from jax.experimental.pallas import tpu as pltpu
from jax.sharding import PartitionSpec as P


NORM_EPS = 1e-5
LOG2E = 1.4426950408889634
HIDE = -(1 << 30)
VMEM_LIMIT = 60 << 20
TURNS = [int(c) for c in '012001010212102201100121202021010212120201102121202']


def norm_kernel(*refs, joined):
    if joined:
        base_ref, pair_ref, came_ref, last_ref, bias_ref, gain_ref, shift_ref, sum_ref, norm_ref = refs
        summed = pair_ref[...].astype(jnp.float32) + came_ref[...].astype(jnp.float32) + last_ref[...].astype(jnp.float32)
        kept = (base_ref[...].astype(jnp.float32) + summed + bias_ref[...].astype(jnp.float32)).astype(jnp.bfloat16)
        sum_ref[...] = kept
    else:
        base_ref, gain_ref, shift_ref, norm_ref = refs
        kept = base_ref[...]
    values = kept.astype(jnp.float32)
    centered = values - jnp.mean(values, axis=-1, keepdims=True)
    variance = jnp.mean(centered * centered, axis=-1, keepdims=True)
    scaled = centered * lax.rsqrt(variance + NORM_EPS)
    norm_ref[...] = (scaled * gain_ref[...].astype(jnp.float32) + shift_ref[...].astype(jnp.float32)).astype(jnp.bfloat16)


def normalize(base, seq, terms, bias, norms, layer, which, rows=32):
    part, model = base.shape[-2:]
    line = pl.BlockSpec((rows, model), lambda i: (i, 0))
    first = line if base.ndim == 2 else pl.BlockSpec((None, rows, model), lambda i: (seq, i, 0))
    vector = lambda at: pl.BlockSpec((None, 1, model), lambda i: (at, 0, 0))
    scale_specs = [vector(4 * layer + which), vector(4 * layer + which + 1)]
    scales = [norms, norms]
    whole = jax.ShapeDtypeStruct((part, model), jnp.bfloat16)
    if terms is None:
        specs, args, outs = [first], [base], [whole]
    else:
        bias, bias_at = bias
        specs, args, outs = [first, line, line, line, vector(bias_at)], [base, *terms, bias], [whole, whole]
    return pl.pallas_call(
        functools.partial(norm_kernel, joined=terms is not None),
        grid=(part // rows,),
        in_specs=specs + scale_specs,
        out_specs=[line] * len(outs),
        out_shape=outs,
        compiler_params=pltpu.CompilerParams(dimension_semantics=('arbitrary',), vmem_limit_bytes=VMEM_LIMIT),
        cost_estimate=pl.CostEstimate(flops=8 * part * model, bytes_accessed=2 * (len(args) + len(outs)) * part * model, transcendentals=0),
        name='norm',
    )(*args, *scales)


def qkv_kernel(x_ref, cos_ref, sin_ref, wq_ref, wk_ref, wv_ref, bq_ref, bk_ref, bv_ref, q_ref, k_ref, v_ref):
    head_dim = cos_ref.shape[-1]
    acts = x_ref[...]
    cos_b = cos_ref[...]
    lane = lax.broadcasted_iota(jnp.int32, cos_b.shape, 1)
    sin_b = jnp.where(lane < head_dim // 2, -sin_ref[...], sin_ref[...])

    def rotary(values):
        return (values * cos_b + pltpu.roll(values, head_dim // 2, 1) * sin_b).astype(jnp.bfloat16)

    query = jnp.dot(acts, wq_ref[...], preferred_element_type=jnp.float32) + bq_ref[...].astype(jnp.float32)
    for head in range(query.shape[1] // head_dim):
        cols = slice(head * head_dim, (head + 1) * head_dim)
        q_ref[:, cols] = rotary(query[:, cols])
    weight_kv = jnp.concatenate([wk_ref[...], wv_ref[...]], axis=1)
    key_value = jnp.dot(acts, weight_kv, preferred_element_type=jnp.float32)
    k_ref[...] = rotary(key_value[:, :head_dim] + bk_ref[...].astype(jnp.float32))
    v_ref[...] = (key_value[:, head_dim:] + bv_ref[...].astype(jnp.float32)).astype(jnp.bfloat16)


def qkv_project(acts, cos_tab, sin_tab, w_q, w_k, w_v, b_q, b_k, b_v, layer, seq, rows=256):
    chunk, model = acts.shape
    head_dim = cos_tab.shape[-1]
    q_cols = w_q.shape[2]
    kv_cols = w_k.shape[2]
    row_block = lambda cols: pl.BlockSpec((rows, cols), lambda i: (i, 0))
    table = pl.BlockSpec((None, rows, head_dim), lambda i: (seq, i, 0))
    weight = lambda cols: pl.BlockSpec((None, model, cols), lambda i: (layer, 0, 0))
    bias = lambda cols: pl.BlockSpec((None, 1, cols), lambda i: (layer, 0, 0))
    return pl.pallas_call(
        qkv_kernel,
        grid=(chunk // rows,),
        in_specs=[row_block(model), table, table, weight(q_cols), weight(kv_cols), weight(kv_cols), bias(q_cols), bias(kv_cols), bias(kv_cols)],
        out_specs=[row_block(q_cols), row_block(kv_cols), row_block(kv_cols)],
        out_shape=[jax.ShapeDtypeStruct((chunk, cols), jnp.bfloat16) for cols in (q_cols, kv_cols, kv_cols)],
        compiler_params=pltpu.CompilerParams(dimension_semantics=('arbitrary',), vmem_limit_bytes=VMEM_LIMIT),
        cost_estimate=pl.CostEstimate(flops=2 * chunk * model * (q_cols + 2 * kv_cols), bytes_accessed=2 * (chunk + q_cols + 2 * kv_cols) * model, transcendentals=0),
        name='qkv_rotary',
    )(acts, cos_tab, sin_tab, w_q, w_k, w_v, b_q[:, None, :], b_k[:, None, :], b_v[:, None, :])


def attention_kernel(start_ref, q_ref, kn_ref, vn_ref, ko_ref, vo_ref, held_ref, o_ref, score_ref, *, seq, group, key_block, new_block):
    rows = q_ref.shape[0]
    head_dim = kn_ref.shape[1]
    window = ko_ref.shape[0]
    block = pl.program_id(0)
    start = start_ref[seq]
    scale = head_dim ** -0.5 * LOG2E
    query = jnp.concatenate([q_ref[:, g * head_dim:(g + 1) * head_dim] for g in range(group)], axis=0)
    token = block * rows + lax.broadcasted_iota(jnp.int32, (rows, 1), 0)
    token = jnp.concatenate([token] * group, axis=0)
    oldest = start + token - window
    top_shape = (rows * group, 128)

    def lane_max(values, top):
        for i in range(values.shape[1] // 128):
            top = jnp.maximum(top, values[:, i * 128:(i + 1) * 128])
        return top

    def lane_sum(values, total):
        for i in range(values.shape[1] // 128):
            total = total + values[:, i * 128:(i + 1) * 128]
        return total

    contract = (((1,), (1,)), ((), ()))

    def score_old(step, top):
        at = pl.multiple_of(step * key_block, key_block)
        values = lax.dot_general(query, ko_ref[pl.ds(at, key_block), :], contract, preferred_element_type=jnp.float32)
        held = held_ref[:, pl.ds(at, key_block)]
        held = jnp.where((held >= 0) & (held < start), held, HIDE)
        values = jnp.where(held > oldest, values, -jnp.inf)
        score_ref[:, pl.ds(at, key_block)] = values
        return lane_max(values, top)

    def score_new(step, top):
        at = pl.multiple_of(step * new_block, new_block)
        values = lax.dot_general(query, kn_ref[pl.ds(at, new_block), :], contract, preferred_element_type=jnp.float32)
        fresh = at + lax.broadcasted_iota(jnp.int32, (1, new_block), 1)
        values = jnp.where(fresh <= token, values, -jnp.inf)
        score_ref[:, pl.ds(pl.multiple_of(window + at, new_block), new_block)] = values
        return lane_max(values, top)

    old_steps = (jnp.minimum(start, window) + key_block - 1) // key_block
    new_steps = (block * rows + rows + new_block - 1) // new_block
    top = jnp.full(top_shape, -jnp.inf, jnp.float32)
    top = lax.fori_loop(0, old_steps, score_old, top)
    top = lax.fori_loop(0, new_steps, score_new, top)
    top = jnp.max(top, axis=1, keepdims=True)

    def weigh(at, size, value_ref, value_at, carry):
        total, mixed = carry
        weights = jnp.exp2((score_ref[:, pl.ds(at, size)] - top) * scale)
        total = lane_sum(weights, total)
        mixed = mixed + jnp.dot(weights.astype(jnp.bfloat16), value_ref[pl.ds(value_at, size), :], preferred_element_type=jnp.float32)
        return total, mixed

    def mix_old(step, carry):
        at = pl.multiple_of(step * key_block, key_block)
        return weigh(at, key_block, vo_ref, at, carry)

    def mix_new(step, carry):
        at = pl.multiple_of(step * new_block, new_block)
        return weigh(pl.multiple_of(window + at, new_block), new_block, vn_ref, at, carry)

    carry = (jnp.zeros(top_shape, jnp.float32), jnp.zeros((rows * group, head_dim), jnp.float32))
    carry = lax.fori_loop(0, old_steps, mix_old, carry)
    total, mixed = lax.fori_loop(0, new_steps, mix_new, carry)
    mixed = (mixed / jnp.sum(total, axis=1, keepdims=True)).astype(jnp.bfloat16)
    for g in range(group):
        o_ref[:, g * head_dim:(g + 1) * head_dim] = mixed[g * rows:(g + 1) * rows]


def attend(query, key_new, value_new, key_cache, value_cache, held, start_pos, layer, seq, rows=256, key_block=2048, new_block=512):
    chunk, q_cols = query.shape
    window, head_dim = key_cache.shape[2:]
    group = q_cols // head_dim
    keys = window + chunk
    whole = pl.BlockSpec((chunk, head_dim), lambda i, *_: (0, 0))
    cache = pl.BlockSpec((None, None, window, head_dim), lambda i, *_: (layer, seq, 0, 0))
    return pl.pallas_call(
        functools.partial(attention_kernel, seq=seq, group=group, key_block=key_block, new_block=new_block),
        grid_spec=pltpu.PrefetchScalarGridSpec(
            num_scalar_prefetch=1,
            grid=(chunk // rows,),
            in_specs=[pl.BlockSpec((rows, q_cols), lambda i, *_: (i, 0)), whole, whole, cache, cache, pl.BlockSpec((None, 1, window), lambda i, *_: (seq, 0, 0))],
            out_specs=pl.BlockSpec((rows, q_cols), lambda i, *_: (i, 0)),
            scratch_shapes=[pltpu.VMEM((rows * group, keys), jnp.float32)],
        ),
        out_shape=jax.ShapeDtypeStruct((chunk, q_cols), jnp.bfloat16),
        compiler_params=pltpu.CompilerParams(dimension_semantics=('arbitrary',), vmem_limit_bytes=VMEM_LIMIT),
        cost_estimate=pl.CostEstimate(flops=8 * chunk * q_cols * keys, bytes_accessed=4 * (window + chunk) * head_dim + 4 * chunk * q_cols, transcendentals=0),
        name='attend',
    )(start_pos, query, key_new, value_new, key_cache, value_cache, held)


def project_kernel(table_ref, acts_ref, weight_ref, *refs, shards, joined):
    part = acts_ref.shape[0] // table_ref.shape[0]
    first = shards if joined is None else 0
    rows = [acts_ref[pl.ds(pl.multiple_of(table_ref[first + i] * part, part), part), :] for i in range(shards)]
    total = jnp.dot(jnp.concatenate(rows, axis=0), weight_ref[...], preferred_element_type=jnp.float32)
    if joined is None:
        refs[0][...] = total.astype(jnp.bfloat16)
    else:
        lead_ref, kept_ref, sent_ref = refs
        total = (total + lead_ref[...].astype(jnp.float32)).astype(jnp.bfloat16)
        kept_ref[...] = total[:total.shape[0] // 2]
        sent_ref[...] = total[total.shape[0] // 2:]


def project_rows(table, acts, weight, layer, lead, cols):
    chunk, depth = acts.shape
    model = weight.shape[2]
    half = chunk // 2
    out = lambda rows: pl.BlockSpec((rows, cols), lambda i, *_: (0, i))
    shape = lambda rows: jax.ShapeDtypeStruct((rows, model), jnp.bfloat16)
    in_specs = [pl.BlockSpec((chunk, depth), lambda i, *_: (0, 0)), pl.BlockSpec((None, depth, cols), lambda i, *_: (layer, 0, i))]
    args = [table, acts, weight]
    if lead is None:
        out_specs, out_shape = [out(half)], [shape(half)]
    else:
        in_specs.append(out(half))
        args.append(lead)
        out_specs, out_shape = [out(half // 2)] * 2, [shape(half // 2)] * 2
    return pl.pallas_call(
        functools.partial(project_kernel, shards=table.shape[0] // 2, joined=None if lead is None else True),
        grid_spec=pltpu.PrefetchScalarGridSpec(num_scalar_prefetch=1, grid=(model // cols,), in_specs=in_specs, out_specs=out_specs),
        out_shape=out_shape,
        compiler_params=pltpu.CompilerParams(dimension_semantics=('arbitrary',), vmem_limit_bytes=VMEM_LIMIT),
        cost_estimate=pl.CostEstimate(flops=2 * half * depth * model, bytes_accessed=2 * (chunk * depth + depth * model + half * model), transcendentals=0),
        name='project_rows',
    )(*args)


def expand_kernel(x_ref, weight_ref, bias_ref, out_ref):
    lifted = jnp.dot(x_ref[...], weight_ref[...], preferred_element_type=jnp.float32) + bias_ref[...].astype(jnp.float32)
    out_ref[...] = jax.nn.gelu(lifted, approximate=True).astype(jnp.bfloat16)


def expand_rows(acts, weight, bias, layer, rows=512, cols=256):
    chunk, model = acts.shape
    width = weight.shape[2]
    return pl.pallas_call(
        expand_kernel,
        grid=(chunk // rows, width // cols),
        in_specs=[pl.BlockSpec((rows, model), lambda i, j: (i, 0)), pl.BlockSpec((None, model, cols), lambda i, j: (layer, 0, j)), pl.BlockSpec((None, 1, cols), lambda i, j: (layer, 0, j))],
        out_specs=pl.BlockSpec((rows, cols), lambda i, j: (i, j)),
        out_shape=jax.ShapeDtypeStruct((chunk, width), jnp.bfloat16),
        compiler_params=pltpu.CompilerParams(dimension_semantics=('arbitrary', 'arbitrary'), vmem_limit_bytes=VMEM_LIMIT),
        cost_estimate=pl.CostEstimate(flops=2 * chunk * model * width, bytes_accessed=2 * (chunk * model + 2 * model * width + chunk * width), transcendentals=0),
        name='expand',
    )(acts, weight, bias)


def cache_kernel(start_ref, ko_ref, vo_ref, kn_ref, vn_ref, kout_ref, vout_ref, ring_ref):
    window, head_dim = ko_ref.shape
    chunk = kn_ref.shape[0]
    pad = 16
    span = chunk + pad
    first = lax.rem(start_ref[pl.program_id(1)], window)
    base = pl.multiple_of((first // pad) * pad, pad)
    inner = first - base
    line = lax.broadcasted_iota(jnp.int32, (span, head_dim), 0)
    for old_ref, new_ref, out_ref in ((ko_ref, kn_ref, kout_ref), (vo_ref, vn_ref, vout_ref)):
        ring_ref[0:window] = old_ref[...]
        ring_ref[window:window + span] = old_ref[0:span]
        fresh = jnp.concatenate([new_ref[...].astype(jnp.float32), jnp.zeros((pad, head_dim), jnp.float32)], axis=0)
        fresh = pltpu.roll(fresh, inner, 0)
        kept = ring_ref[pl.ds(base, span), :].astype(jnp.float32)
        mine = (line >= inner) & (line < inner + chunk)
        ring_ref[pl.ds(base, span), :] = jnp.where(mine, fresh, kept).astype(jnp.bfloat16)
        out_ref[span:window] = ring_ref[span:window]
        wrapped = ring_ref[window:window + span].astype(jnp.float32)
        plain = ring_ref[0:span].astype(jnp.float32)
        out_ref[0:span] = jnp.where(line < first + chunk - window, wrapped, plain).astype(jnp.bfloat16)


def update_caches(start_pos, key_cache, value_cache, key_new, value_new):
    layers, seqs, window, head_dim = key_cache.shape
    chunk = key_new.shape[2]
    old = pl.BlockSpec((None, None, window, head_dim), lambda i, j, *_: (i, j, 0, 0))
    new = pl.BlockSpec((None, None, chunk, head_dim), lambda i, j, *_: (i, j, 0, 0))
    return pl.pallas_call(
        cache_kernel,
        grid_spec=pltpu.PrefetchScalarGridSpec(
            num_scalar_prefetch=1,
            grid=(layers, seqs),
            in_specs=[old, old, new, new],
            out_specs=[old, old],
            scratch_shapes=[pltpu.VMEM((window + chunk + 16, head_dim), jnp.bfloat16)],
        ),
        out_shape=[jax.ShapeDtypeStruct(key_cache.shape, jnp.bfloat16)] * 2,
        compiler_params=pltpu.CompilerParams(dimension_semantics=('arbitrary', 'arbitrary'), vmem_limit_bytes=VMEM_LIMIT),
        cost_estimate=pl.CostEstimate(flops=1 << 24, bytes_accessed=8 * layers * seqs * window * head_dim, transcendentals=0),
        name='write_caches',
    )(start_pos, key_cache, value_cache, key_new, value_new)


def solution(mesh):
    row_spec = P('dp', 'tp', None)
    cache_spec = P(None, 'dp', None, 'tp', None)
    col_spec = P(None, None, 'tp')
    bias_spec = P(None, 'tp')
    in_specs = (row_spec, P('dp'), P('dp', None, None), P('dp', None, None), cache_spec, cache_spec, P('dp', None), P(), col_spec, bias_spec, col_spec, bias_spec, col_spec, bias_spec, P(None, 'tp', None), P(), col_spec, bias_spec, P(None, 'tp', None), P())
    out_specs = (row_spec, cache_spec, cache_spec, P('dp', None))
    count = mesh.shape['tp']
    first_axis = lambda core: 1 + core
    pairs_core = [(d, d ^ 1) for d in range(count)]
    pairs_first = [(d, ((d // 2) ^ first_axis(d % 2)) * 2 + d % 2) for d in range(count)]
    pairs_second = [(d, ((d // 2) ^ (3 - first_axis(d % 2))) * 2 + d % 2) for d in range(count)]

    def device_step(tokens, start_pos, cos_tab, sin_tab, key_cache, value_cache, slot_pos, norm_params, w_q, b_q, w_k, b_k, w_v, b_v, w_o, b_o, w_up, b_up, w_down, b_down):
        num_seqs, part, model = tokens.shape
        chunk = cos_tab.shape[1]
        head_dim = cos_tab.shape[2]
        layers = key_cache.shape[0]
        window = key_cache.shape[2]
        keys_in = key_cache.reshape(layers, num_seqs, window, head_dim)
        values_in = value_cache.reshape(layers, num_seqs, window, head_dim)
        held = slot_pos[:, None, :]
        me = lax.axis_index('tp')
        chip, core = me // 2, me % 2
        near, far = 1 + core, 2 - core
        mine = [chip ^ flip for flip in (0, far, near, 3)]
        theirs = [chip ^ flip for flip in (0, near, far, 3)]
        order = [c * 2 + core for c in mine] + [c * 2 + 1 - core for c in theirs]
        table = jnp.stack(order).astype(jnp.int32)
        norms = norm_params.reshape(-1, 1, model)
        out_bias = b_o[:, None, :]
        down_bias = b_down[:, None, :]
        latest = [None]
        turn = [0]

        def item(compute, *values):
            if latest[0] is not None:
                values = lax.optimization_barrier((*values, latest[0]))[:-1]
            results = compute(*values)
            latest[0] = results[0]
            return results

        def send(value, pairs):
            return lax.ppermute(value, 'tp', pairs)

        def gather(value):
            return lax.all_gather(value, 'tp', axis=0, tiled=True)

        up_bias = b_up[:, None, :]

        def add_came(kept, came):
            return ((kept[part:].astype(jnp.float32) + came[part:].astype(jnp.float32)).astype(jnp.bfloat16),)

        def scatter_sum(lead, acts, weight, layer, cols):
            lead = send(lead, pairs_core)
            yield
            kept, sent = item(lambda lead: project_rows(table, acts, weight, layer, lead, cols), lead)
            came = send(sent, pairs_first)
            yield
            onward, = item(add_came, kept, came)
            last = send(onward, pairs_second)
            yield
            return kept, came, last

        def attention(gathered, layer, seq):
            query, key_new, value_new = qkv_project(gathered, cos_tab, sin_tab, w_q, w_k, w_v, b_q, b_k, b_v, layer, seq)
            fresh_keys[layer][seq] = key_new
            fresh_values[layer][seq] = value_new
            mixed = attend(query, key_new, value_new, keys_in, values_in, held, start_pos, layer, seq)
            lead, = project_rows(table, mixed, w_o, layer, None, 1024)
            return lead, mixed

        def expand(gathered, layer):
            active = expand_rows(gathered, w_up, up_bias, layer)
            lead, = project_rows(table, active, w_down, layer, None, 512)
            return lead, active

        def finish(middle, kept, came, last):
            summed = kept[:part].astype(jnp.float32) + came[:part].astype(jnp.float32) + last.astype(jnp.float32)
            return ((middle.astype(jnp.float32) + summed + b_down[layers - 1].astype(jnp.float32)).astype(jnp.bfloat16),)

        def join(base, *terms, bias, layer, which):
            middle, normed = normalize(base, seq_of[0], terms, (bias, layer), norms, layer + which // 4, which % 4)
            return normed, middle

        seq_of = [0]
        fresh_keys = [[None] * num_seqs for _ in range(layers)]
        fresh_values = [[None] * num_seqs for _ in range(layers)]
        hidden_out = [None] * num_seqs

        def stream(seq):
            base = tokens
            normed, = item(lambda: normalize(base, seq, None, None, norms, 0, 0))
            for layer in range(layers):
                gathered = gather(normed)
                yield
                lead, own = item(functools.partial(attention, layer=layer, seq=seq), gathered)
                terms = yield from scatter_sum(lead, own, w_o, layer, 1024)
                seq_of[0] = seq
                normed, middle = item(lambda *terms: join(base, *terms, bias=out_bias, layer=layer, which=2), *terms)
                gathered = gather(normed)
                yield
                lead, own = item(functools.partial(expand, layer=layer), gathered)
                terms = yield from scatter_sum(lead, own, w_down, layer, 512)
                if layer + 1 < layers:
                    seq_of[0] = seq
                    normed, base = item(lambda *terms: join(middle, *terms, bias=down_bias, layer=layer, which=4), *terms)
                else:
                    hidden_out[seq], = item(finish, middle, *terms)
            yield

        streams = [stream(seq) for seq in range(num_seqs)]
        for step, seq in enumerate(TURNS):
            turn[0] = step
            next(streams[seq])
        fresh_keys = [jnp.stack(k) for k in fresh_keys]
        fresh_values = [jnp.stack(v) for v in fresh_values]
        key_out, value_out = update_caches(start_pos, keys_in, values_in, jnp.stack(fresh_keys), jnp.stack(fresh_values))
        first_slot = start_pos % window
        offset = (jnp.arange(window)[None, :] - first_slot[:, None]) % window
        pos_out = jnp.where(offset < chunk, start_pos[:, None] + offset, slot_pos)
        return jnp.stack(hidden_out), key_out.reshape(key_cache.shape), value_out.reshape(value_cache.shape), pos_out

    return jax.shard_map(device_step, mesh=mesh, in_specs=in_specs, out_specs=out_specs, check_vma=False)
```

```python
import functools

import jax
import jax.numpy as jnp
from jax import lax
from jax.experimental import pallas as pl
from jax.experimental.pallas import tpu as pltpu
from jax.sharding import PartitionSpec as P


NORM_EPS = 1e-5
LOG2E = 1.4426950408889634
HIDE = -(1 << 30)
VMEM_LIMIT = 60 << 20
TURNS = [int(c) for c in '012001010212102201100121202021010212120201102121202']


def norm_kernel(*refs, joined):
    if joined:
        base_ref, pair_ref, came_ref, last_ref, bias_ref, gain_ref, shift_ref, sum_ref, norm_ref = refs
        summed = pair_ref[...].astype(jnp.float32) + came_ref[...].astype(jnp.float32) + last_ref[...].astype(jnp.float32)
        kept = (base_ref[...].astype(jnp.float32) + summed + bias_ref[...].astype(jnp.float32)).astype(jnp.bfloat16)
        sum_ref[...] = kept
    else:
        base_ref, gain_ref, shift_ref, norm_ref = refs
        kept = base_ref[...]
    values = kept.astype(jnp.float32)
    centered = values - jnp.mean(values, axis=-1, keepdims=True)
    variance = jnp.mean(centered * centered, axis=-1, keepdims=True)
    scaled = centered * lax.rsqrt(variance + NORM_EPS)
    norm_ref[...] = (scaled * gain_ref[...].astype(jnp.float32) + shift_ref[...].astype(jnp.float32)).astype(jnp.bfloat16)


def normalize(base, seq, terms, bias, norms, layer, which, rows=64):
    part, model = base.shape[-2:]
    line = pl.BlockSpec((rows, model), lambda i: (i, 0))
    first = line if base.ndim == 2 else pl.BlockSpec((None, rows, model), lambda i: (seq, i, 0))
    vector = lambda at: pl.BlockSpec((None, 1, model), lambda i: (at, 0, 0))
    scale_specs = [vector(4 * layer + which), vector(4 * layer + which + 1)]
    scales = [norms, norms]
    whole = jax.ShapeDtypeStruct((part, model), jnp.bfloat16)
    if terms is None:
        specs, args, outs = [first], [base], [whole]
    else:
        bias, bias_at = bias
        specs, args, outs = [first, line, line, line, vector(bias_at)], [base, *terms, bias], [whole, whole]
    return pl.pallas_call(
        functools.partial(norm_kernel, joined=terms is not None),
        grid=(part // rows,),
        in_specs=specs + scale_specs,
        out_specs=[line] * len(outs),
        out_shape=outs,
        compiler_params=pltpu.CompilerParams(dimension_semantics=('arbitrary',), vmem_limit_bytes=VMEM_LIMIT),
        cost_estimate=pl.CostEstimate(flops=8 * part * model, bytes_accessed=2 * (len(args) + len(outs)) * part * model, transcendentals=0),
        name='norm',
    )(*args, *scales)


def qkv_kernel(x_ref, cos_ref, sin_ref, wq_ref, wk_ref, wv_ref, bq_ref, bk_ref, bv_ref, q_ref, k_ref, v_ref):
    head_dim = cos_ref.shape[-1]
    acts = x_ref[...]
    cos_b = cos_ref[...]
    lane = lax.broadcasted_iota(jnp.int32, cos_b.shape, 1)
    sin_b = jnp.where(lane < head_dim // 2, -sin_ref[...], sin_ref[...])

    def rotary(values):
        return (values * cos_b + pltpu.roll(values, head_dim // 2, 1) * sin_b).astype(jnp.bfloat16)

    query = jnp.dot(acts, wq_ref[...], preferred_element_type=jnp.float32) + bq_ref[...].astype(jnp.float32)
    for head in range(query.shape[1] // head_dim):
        cols = slice(head * head_dim, (head + 1) * head_dim)
        q_ref[:, cols] = rotary(query[:, cols])
    weight_kv = jnp.concatenate([wk_ref[...], wv_ref[...]], axis=1)
    key_value = jnp.dot(acts, weight_kv, preferred_element_type=jnp.float32)
    k_ref[...] = rotary(key_value[:, :head_dim] + bk_ref[...].astype(jnp.float32))
    v_ref[...] = (key_value[:, head_dim:] + bv_ref[...].astype(jnp.float32)).astype(jnp.bfloat16)


def qkv_project(acts, cos_tab, sin_tab, w_q, w_k, w_v, b_q, b_k, b_v, layer, seq, rows=256):
    chunk, model = acts.shape
    head_dim = cos_tab.shape[-1]
    q_cols = w_q.shape[2]
    kv_cols = w_k.shape[2]
    row_block = lambda cols: pl.BlockSpec((rows, cols), lambda i: (i, 0))
    table = pl.BlockSpec((None, rows, head_dim), lambda i: (seq, i, 0))
    weight = lambda cols: pl.BlockSpec((None, model, cols), lambda i: (layer, 0, 0))
    bias = lambda cols: pl.BlockSpec((None, 1, cols), lambda i: (layer, 0, 0))
    return pl.pallas_call(
        qkv_kernel,
        grid=(chunk // rows,),
        in_specs=[row_block(model), table, table, weight(q_cols), weight(kv_cols), weight(kv_cols), bias(q_cols), bias(kv_cols), bias(kv_cols)],
        out_specs=[row_block(q_cols), row_block(kv_cols), row_block(kv_cols)],
        out_shape=[jax.ShapeDtypeStruct((chunk, cols), jnp.bfloat16) for cols in (q_cols, kv_cols, kv_cols)],
        compiler_params=pltpu.CompilerParams(dimension_semantics=('arbitrary',), vmem_limit_bytes=VMEM_LIMIT),
        cost_estimate=pl.CostEstimate(flops=2 * chunk * model * (q_cols + 2 * kv_cols), bytes_accessed=2 * (chunk + q_cols + 2 * kv_cols) * model, transcendentals=0),
        name='qkv_rotary',
    )(acts, cos_tab, sin_tab, w_q, w_k, w_v, b_q[:, None, :], b_k[:, None, :], b_v[:, None, :])


def attention_kernel(start_ref, q_ref, kn_ref, vn_ref, ko_ref, vo_ref, held_ref, o_ref, score_ref, *, seq, group, key_block, new_block):
    rows = q_ref.shape[0]
    head_dim = kn_ref.shape[1]
    window = ko_ref.shape[0]
    block = pl.program_id(0)
    start = start_ref[seq]
    scale = head_dim ** -0.5 * LOG2E
    query = jnp.concatenate([q_ref[:, g * head_dim:(g + 1) * head_dim] for g in range(group)], axis=0)
    token = block * rows + lax.broadcasted_iota(jnp.int32, (rows, 1), 0)
    token = jnp.concatenate([token] * group, axis=0)
    oldest = start + token - window
    top_shape = (rows * group, 128)

    def lane_max(values, top):
        for i in range(values.shape[1] // 128):
            top = jnp.maximum(top, values[:, i * 128:(i + 1) * 128])
        return top

    def lane_sum(values, total):
        for i in range(values.shape[1] // 128):
            total = total + values[:, i * 128:(i + 1) * 128]
        return total

    contract = (((1,), (1,)), ((), ()))

    def score_old(step, top):
        at = pl.multiple_of(step * key_block, key_block)
        values = lax.dot_general(query, ko_ref[pl.ds(at, key_block), :], contract, preferred_element_type=jnp.float32)
        held = held_ref[:, pl.ds(at, key_block)]
        held = jnp.where((held >= 0) & (held < start), held, HIDE)
        values = jnp.where(held > oldest, values, -jnp.inf)
        score_ref[:, pl.ds(at, key_block)] = values
        return lane_max(values, top)

    def score_new(step, top):
        at = pl.multiple_of(step * new_block, new_block)
        values = lax.dot_general(query, kn_ref[pl.ds(at, new_block), :], contract, preferred_element_type=jnp.float32)
        fresh = at + lax.broadcasted_iota(jnp.int32, (1, new_block), 1)
        values = jnp.where(fresh <= token, values, -jnp.inf)
        score_ref[:, pl.ds(pl.multiple_of(window + at, new_block), new_block)] = values
        return lane_max(values, top)

    old_steps = (jnp.minimum(start, window) + key_block - 1) // key_block
    new_steps = (block * rows + rows + new_block - 1) // new_block
    top = jnp.full(top_shape, -jnp.inf, jnp.float32)
    top = lax.fori_loop(0, old_steps, score_old, top)
    top = lax.fori_loop(0, new_steps, score_new, top)
    top = jnp.max(top, axis=1, keepdims=True)

    def weigh(at, size, value_ref, value_at, carry):
        total, mixed = carry
        weights = jnp.exp2((score_ref[:, pl.ds(at, size)] - top) * scale)
        total = lane_sum(weights, total)
        mixed = mixed + jnp.dot(weights.astype(jnp.bfloat16), value_ref[pl.ds(value_at, size), :], preferred_element_type=jnp.float32)
        return total, mixed

    def mix_old(step, carry):
        at = pl.multiple_of(step * key_block, key_block)
        return weigh(at, key_block, vo_ref, at, carry)

    def mix_new(step, carry):
        at = pl.multiple_of(step * new_block, new_block)
        return weigh(pl.multiple_of(window + at, new_block), new_block, vn_ref, at, carry)

    carry = (jnp.zeros(top_shape, jnp.float32), jnp.zeros((rows * group, head_dim), jnp.float32))
    carry = lax.fori_loop(0, old_steps, mix_old, carry)
    total, mixed = lax.fori_loop(0, new_steps, mix_new, carry)
    mixed = (mixed / jnp.sum(total, axis=1, keepdims=True)).astype(jnp.bfloat16)
    for g in range(group):
        o_ref[:, g * head_dim:(g + 1) * head_dim] = mixed[g * rows:(g + 1) * rows]


def attend(query, key_new, value_new, key_cache, value_cache, held, start_pos, layer, seq, rows=256, key_block=2048, new_block=512):
    chunk, q_cols = query.shape
    window, head_dim = key_cache.shape[2:]
    group = q_cols // head_dim
    keys = window + chunk
    whole = pl.BlockSpec((chunk, head_dim), lambda i, *_: (0, 0))
    cache = pl.BlockSpec((None, None, window, head_dim), lambda i, *_: (layer, seq, 0, 0))
    return pl.pallas_call(
        functools.partial(attention_kernel, seq=seq, group=group, key_block=key_block, new_block=new_block),
        grid_spec=pltpu.PrefetchScalarGridSpec(
            num_scalar_prefetch=1,
            grid=(chunk // rows,),
            in_specs=[pl.BlockSpec((rows, q_cols), lambda i, *_: (i, 0)), whole, whole, cache, cache, pl.BlockSpec((None, 1, window), lambda i, *_: (seq, 0, 0))],
            out_specs=pl.BlockSpec((rows, q_cols), lambda i, *_: (i, 0)),
            scratch_shapes=[pltpu.VMEM((rows * group, keys), jnp.float32)],
        ),
        out_shape=jax.ShapeDtypeStruct((chunk, q_cols), jnp.bfloat16),
        compiler_params=pltpu.CompilerParams(dimension_semantics=('arbitrary',), vmem_limit_bytes=VMEM_LIMIT),
        cost_estimate=pl.CostEstimate(flops=8 * chunk * q_cols * keys, bytes_accessed=4 * (window + chunk) * head_dim + 4 * chunk * q_cols, transcendentals=0),
        name='attend',
    )(start_pos, query, key_new, value_new, key_cache, value_cache, held)


def stream_tile(weight_ref, ring_ref, sem_ref, step, steps, layer, tiles):
    slots, _, cols = ring_ref.shape

    def copy(at):
        slot = lax.rem(at, slots)
        columns = pl.ds(pl.multiple_of(lax.rem(at, tiles) * cols, cols), cols)
        return pltpu.make_async_copy(weight_ref.at[layer, :, columns], ring_ref.at[slot], sem_ref.at[slot])

    @pl.when(step == 0)
    def _():
        for i in range(min(slots - 1, steps)):
            copy(jnp.int32(i)).start()

    @pl.when(step + slots - 1 < steps)
    def _():
        copy(step + slots - 1).start()

    copy(step).wait()
    return ring_ref[lax.rem(step, slots)]


def project_kernel(table_ref, *refs, shards, joined, layer, steps):
    acts_refs, (weight_ref, *refs), (ring_ref, sem_ref) = refs[:shards], refs[shards:-2], refs[-2:]
    weight = stream_tile(weight_ref, ring_ref, sem_ref, pl.program_id(0), steps, layer, steps)
    total = jnp.dot(jnp.concatenate([ref[...] for ref in acts_refs], axis=0), weight, preferred_element_type=jnp.float32)
    if not joined:
        refs[0][...] = total.astype(jnp.bfloat16)
    else:
        lead_ref, kept_ref, sent_ref = refs
        total = (total + lead_ref[...].astype(jnp.float32)).astype(jnp.bfloat16)
        kept_ref[...] = total[:total.shape[0] // 2]
        sent_ref[...] = total[total.shape[0] // 2:]


def project_rows(table, acts, weight, layer, lead, cols, slots=4):
    chunk, depth = acts.shape
    model = weight.shape[2]
    half = chunk // 2
    shards = table.shape[0] // 2
    part = half // shards
    first = shards if lead is None else 0
    out = lambda rows: pl.BlockSpec((rows, cols), lambda i, *_: (0, i))
    shape = lambda rows: jax.ShapeDtypeStruct((rows, model), jnp.bfloat16)
    shard = lambda at: pl.BlockSpec((part, depth), lambda i, places: (places[at], 0))
    in_specs = [shard(first + k) for k in range(shards)] + [pl.BlockSpec(memory_space=pl.ANY)]
    args = [table] + [acts] * shards + [weight]
    if lead is None:
        out_specs, out_shape = [out(half)], [shape(half)]
    else:
        in_specs.append(out(half))
        args.append(lead)
        out_specs, out_shape = [out(half // 2)] * 2, [shape(half // 2)] * 2
    return pl.pallas_call(
        functools.partial(project_kernel, shards=shards, joined=lead is not None, layer=layer, steps=model // cols),
        grid_spec=pltpu.PrefetchScalarGridSpec(
            num_scalar_prefetch=1,
            grid=(model // cols,),
            in_specs=in_specs,
            out_specs=out_specs,
            scratch_shapes=[pltpu.VMEM((slots, depth, cols), jnp.bfloat16), pltpu.SemaphoreType.DMA((slots,))],
        ),
        out_shape=out_shape,
        compiler_params=pltpu.CompilerParams(dimension_semantics=('arbitrary',), vmem_limit_bytes=VMEM_LIMIT),
        cost_estimate=pl.CostEstimate(flops=2 * half * depth * model, bytes_accessed=2 * (half * depth + depth * model + half * model), transcendentals=0),
        name='project_rows',
    )(*args)


def expand_kernel(x_ref, weight_ref, bias_ref, out_ref, ring_ref, sem_ref, *, layer, blocks, tiles):
    step = pl.program_id(0) * tiles + pl.program_id(1)
    weight = stream_tile(weight_ref, ring_ref, sem_ref, step, blocks * tiles, layer, tiles)
    lifted = jnp.dot(x_ref[...], weight, preferred_element_type=jnp.float32) + bias_ref[...].astype(jnp.float32)
    out_ref[...] = jax.nn.gelu(lifted, approximate=True).astype(jnp.bfloat16)


def expand_rows(acts, weight, bias, layer, rows=512, cols=256, slots=4):
    chunk, model = acts.shape
    width = weight.shape[2]
    blocks, tiles = chunk // rows, width // cols
    return pl.pallas_call(
        functools.partial(expand_kernel, layer=layer, blocks=blocks, tiles=tiles),
        grid=(blocks, tiles),
        in_specs=[pl.BlockSpec((rows, model), lambda i, j: (i, 0)), pl.BlockSpec(memory_space=pl.ANY), pl.BlockSpec((None, 1, cols), lambda i, j: (layer, 0, j))],
        out_specs=pl.BlockSpec((rows, cols), lambda i, j: (i, j)),
        scratch_shapes=[pltpu.VMEM((slots, model, cols), jnp.bfloat16), pltpu.SemaphoreType.DMA((slots,))],
        out_shape=jax.ShapeDtypeStruct((chunk, width), jnp.bfloat16),
        compiler_params=pltpu.CompilerParams(dimension_semantics=('arbitrary', 'arbitrary'), vmem_limit_bytes=VMEM_LIMIT),
        cost_estimate=pl.CostEstimate(flops=2 * chunk * model * width, bytes_accessed=2 * (chunk * model + blocks * model * width + chunk * width), transcendentals=0),
        name='expand',
    )(acts, weight, bias)


def cache_kernel(start_ref, ko_ref, vo_ref, kn_ref, vn_ref, kout_ref, vout_ref, ring_ref):
    window, head_dim = ko_ref.shape
    chunk = kn_ref.shape[0]
    pad = 16
    span = chunk + pad
    first = lax.rem(start_ref[pl.program_id(1)], window)
    base = pl.multiple_of((first // pad) * pad, pad)
    inner = first - base
    line = lax.broadcasted_iota(jnp.int32, (span, head_dim), 0)
    for old_ref, new_ref, out_ref in ((ko_ref, kn_ref, kout_ref), (vo_ref, vn_ref, vout_ref)):
        ring_ref[0:window] = old_ref[...]
        ring_ref[window:window + span] = old_ref[0:span]
        fresh = jnp.concatenate([new_ref[...].astype(jnp.float32), jnp.zeros((pad, head_dim), jnp.float32)], axis=0)
        fresh = pltpu.roll(fresh, inner, 0)
        kept = ring_ref[pl.ds(base, span), :].astype(jnp.float32)
        mine = (line >= inner) & (line < inner + chunk)
        ring_ref[pl.ds(base, span), :] = jnp.where(mine, fresh, kept).astype(jnp.bfloat16)
        out_ref[span:window] = ring_ref[span:window]
        wrapped = ring_ref[window:window + span].astype(jnp.float32)
        plain = ring_ref[0:span].astype(jnp.float32)
        out_ref[0:span] = jnp.where(line < first + chunk - window, wrapped, plain).astype(jnp.bfloat16)


def update_caches(start_pos, key_cache, value_cache, key_new, value_new):
    layers, seqs, window, head_dim = key_cache.shape
    chunk = key_new.shape[2]
    old = pl.BlockSpec((None, None, window, head_dim), lambda i, j, *_: (i, j, 0, 0))
    new = pl.BlockSpec((None, None, chunk, head_dim), lambda i, j, *_: (i, j, 0, 0))
    return pl.pallas_call(
        cache_kernel,
        grid_spec=pltpu.PrefetchScalarGridSpec(
            num_scalar_prefetch=1,
            grid=(layers, seqs),
            in_specs=[old, old, new, new],
            out_specs=[old, old],
            scratch_shapes=[pltpu.VMEM((window + chunk + 16, head_dim), jnp.bfloat16)],
        ),
        out_shape=[jax.ShapeDtypeStruct(key_cache.shape, jnp.bfloat16)] * 2,
        compiler_params=pltpu.CompilerParams(dimension_semantics=('arbitrary', 'arbitrary'), vmem_limit_bytes=VMEM_LIMIT),
        cost_estimate=pl.CostEstimate(flops=1 << 24, bytes_accessed=8 * layers * seqs * window * head_dim, transcendentals=0),
        name='write_caches',
    )(start_pos, key_cache, value_cache, key_new, value_new)


def solution(mesh):
    row_spec = P('dp', 'tp', None)
    cache_spec = P(None, 'dp', None, 'tp', None)
    col_spec = P(None, None, 'tp')
    bias_spec = P(None, 'tp')
    in_specs = (row_spec, P('dp'), P('dp', None, None), P('dp', None, None), cache_spec, cache_spec, P('dp', None), P(), col_spec, bias_spec, col_spec, bias_spec, col_spec, bias_spec, P(None, 'tp', None), P(), col_spec, bias_spec, P(None, 'tp', None), P())
    out_specs = (row_spec, cache_spec, cache_spec, P('dp', None))
    count = mesh.shape['tp']
    first_axis = lambda core: 1 + core
    pairs_core = [(d, d ^ 1) for d in range(count)]
    pairs_first = [(d, ((d // 2) ^ first_axis(d % 2)) * 2 + d % 2) for d in range(count)]
    pairs_second = [(d, ((d // 2) ^ (3 - first_axis(d % 2))) * 2 + d % 2) for d in range(count)]

    def device_step(tokens, start_pos, cos_tab, sin_tab, key_cache, value_cache, slot_pos, norm_params, w_q, b_q, w_k, b_k, w_v, b_v, w_o, b_o, w_up, b_up, w_down, b_down):
        num_seqs, part, model = tokens.shape
        chunk = cos_tab.shape[1]
        head_dim = cos_tab.shape[2]
        layers = key_cache.shape[0]
        window = key_cache.shape[2]
        keys_in = key_cache.reshape(layers, num_seqs, window, head_dim)
        values_in = value_cache.reshape(layers, num_seqs, window, head_dim)
        held = slot_pos[:, None, :]
        me = lax.axis_index('tp')
        chip, core = me // 2, me % 2
        near, far = 1 + core, 2 - core
        mine = [chip ^ flip for flip in (0, far, near, 3)]
        theirs = [chip ^ flip for flip in (0, near, far, 3)]
        order = [c * 2 + core for c in mine] + [c * 2 + 1 - core for c in theirs]
        table = jnp.stack(order).astype(jnp.int32)
        norms = norm_params.reshape(-1, 1, model)
        out_bias = b_o[:, None, :]
        down_bias = b_down[:, None, :]
        latest = [None]
        turn = [0]

        def item(compute, *values):
            if latest[0] is not None:
                values = lax.optimization_barrier((*values, latest[0]))[:-1]
            results = compute(*values)
            latest[0] = results[0]
            return results

        def send(value, pairs):
            return lax.ppermute(value, 'tp', pairs)

        def gather(value):
            return lax.all_gather(value, 'tp', axis=0, tiled=True)

        up_bias = b_up[:, None, :]

        def add_came(kept, came):
            return ((kept[part:].astype(jnp.float32) + came[part:].astype(jnp.float32)).astype(jnp.bfloat16),)

        def scatter_sum(lead, acts, weight, layer, cols):
            lead = send(lead, pairs_core)
            yield
            kept, sent = item(lambda lead: project_rows(table, acts, weight, layer, lead, cols), lead)
            came = send(sent, pairs_first)
            yield
            onward, = item(add_came, kept, came)
            last = send(onward, pairs_second)
            yield
            return kept, came, last

        def attention(gathered, layer, seq):
            query, key_new, value_new = qkv_project(gathered, cos_tab, sin_tab, w_q, w_k, w_v, b_q, b_k, b_v, layer, seq)
            fresh_keys[layer][seq] = key_new
            fresh_values[layer][seq] = value_new
            mixed = attend(query, key_new, value_new, keys_in, values_in, held, start_pos, layer, seq)
            lead, = project_rows(table, mixed, w_o, layer, None, 1024)
            return lead, mixed

        def expand(gathered, layer):
            active = expand_rows(gathered, w_up, up_bias, layer)
            lead, = project_rows(table, active, w_down, layer, None, 512)
            return lead, active

        def finish(middle, kept, came, last):
            summed = kept[:part].astype(jnp.float32) + came[:part].astype(jnp.float32) + last.astype(jnp.float32)
            return ((middle.astype(jnp.float32) + summed + b_down[layers - 1].astype(jnp.float32)).astype(jnp.bfloat16),)

        def join(base, *terms, bias, layer, which):
            middle, normed = normalize(base, seq_of[0], terms, (bias, layer), norms, layer + which // 4, which % 4)
            return normed, middle

        seq_of = [0]
        fresh_keys = [[None] * num_seqs for _ in range(layers)]
        fresh_values = [[None] * num_seqs for _ in range(layers)]
        hidden_out = [None] * num_seqs

        def stream(seq):
            base = tokens
            normed, = item(lambda: normalize(base, seq, None, None, norms, 0, 0))
            for layer in range(layers):
                gathered = gather(normed)
                yield
                lead, own = item(functools.partial(attention, layer=layer, seq=seq), gathered)
                terms = yield from scatter_sum(lead, own, w_o, layer, 1024)
                seq_of[0] = seq
                normed, middle = item(lambda *terms: join(base, *terms, bias=out_bias, layer=layer, which=2), *terms)
                gathered = gather(normed)
                yield
                lead, own = item(functools.partial(expand, layer=layer), gathered)
                terms = yield from scatter_sum(lead, own, w_down, layer, 512)
                if layer + 1 < layers:
                    seq_of[0] = seq
                    normed, base = item(lambda *terms: join(middle, *terms, bias=down_bias, layer=layer, which=4), *terms)
                else:
                    hidden_out[seq], = item(finish, middle, *terms)
            yield

        streams = [stream(seq) for seq in range(num_seqs)]
        for step, seq in enumerate(TURNS):
            turn[0] = step
            next(streams[seq])
        fresh_keys = [jnp.stack(k) for k in fresh_keys]
        fresh_values = [jnp.stack(v) for v in fresh_values]
        key_out, value_out = update_caches(start_pos, keys_in, values_in, jnp.stack(fresh_keys), jnp.stack(fresh_values))
        first_slot = start_pos % window
        offset = (jnp.arange(window)[None, :] - first_slot[:, None]) % window
        pos_out = jnp.where(offset < chunk, start_pos[:, None] + offset, slot_pos)
        return jnp.stack(hidden_out), key_out.reshape(key_cache.shape), value_out.reshape(value_cache.shape), pos_out

    return jax.shard_map(device_step, mesh=mesh, in_specs=in_specs, out_specs=out_specs, check_vma=False)
```

```python
import functools

import jax
import jax.numpy as jnp
from jax import lax
from jax.experimental import pallas as pl
from jax.experimental.pallas import tpu as pltpu
from jax.sharding import PartitionSpec as P


NORM_EPS = 1e-5
LOG2E = 1.4426950408889634
HIDE = -(1 << 30)
VMEM_LIMIT = 60 << 20
TURNS = [int(c) for c in '210221212010120201212010120201212010120012102101020']


def norm_kernel(*refs, joined, which):
    if joined:
        base_ref, pair_ref, came_ref, last_ref, bias_ref, scale_ref, sum_ref, norm_ref = refs
        summed = pair_ref[...].astype(jnp.float32) + came_ref[...].astype(jnp.float32) + last_ref[...].astype(jnp.float32)
        kept = (base_ref[...].astype(jnp.float32) + summed + bias_ref[...].astype(jnp.float32)).astype(jnp.bfloat16)
        sum_ref[...] = kept
    else:
        base_ref, scale_ref, norm_ref = refs
        kept = base_ref[...]
    values = kept.astype(jnp.float32)
    centered = values - jnp.mean(values, axis=-1, keepdims=True)
    variance = jnp.mean(centered * centered, axis=-1, keepdims=True)
    scaled = centered * lax.rsqrt(variance + NORM_EPS)
    norm_ref[...] = (scaled * scale_ref[which:which + 1, :].astype(jnp.float32) + scale_ref[which + 1:which + 2, :].astype(jnp.float32)).astype(jnp.bfloat16)


def normalize(base, seq, terms, bias, norms, layer, which, rows=64):
    part, model = base.shape[-2:]
    line = pl.BlockSpec((rows, model), lambda i: (i, 0))
    first = line if base.ndim == 2 else pl.BlockSpec((None, rows, model), lambda i: (seq, i, 0))
    vector = lambda at: pl.BlockSpec((None, 1, model), lambda i: (at, 0, 0))
    scale_specs = [pl.BlockSpec((None, norms.shape[1], model), lambda i: (layer, 0, 0))]
    scales = [norms]
    whole = jax.ShapeDtypeStruct((part, model), jnp.bfloat16)
    if terms is None:
        specs, args, outs = [first], [base], [whole]
    else:
        bias, bias_at = bias
        specs, args, outs = [first, line, line, line, vector(bias_at)], [base, *terms, bias], [whole, whole]
    return pl.pallas_call(
        functools.partial(norm_kernel, joined=terms is not None, which=which),
        grid=(part // rows,),
        in_specs=specs + scale_specs,
        out_specs=[line] * len(outs),
        out_shape=outs,
        compiler_params=pltpu.CompilerParams(dimension_semantics=('arbitrary',), vmem_limit_bytes=VMEM_LIMIT),
        cost_estimate=pl.CostEstimate(flops=8 * part * model, bytes_accessed=2 * (len(args) + len(outs)) * part * model, transcendentals=0),
        name='norm',
    )(*args, *scales)


def qkv_kernel(x_ref, cos_ref, sin_ref, wq_ref, wk_ref, wv_ref, bq_ref, bk_ref, bv_ref, q_ref, k_ref, v_ref):
    head_dim = cos_ref.shape[-1]
    acts = x_ref[...]
    cos_b = cos_ref[...]
    lane = lax.broadcasted_iota(jnp.int32, cos_b.shape, 1)
    sin_b = jnp.where(lane < head_dim // 2, -sin_ref[...], sin_ref[...])

    def rotary(values):
        return (values * cos_b + pltpu.roll(values, head_dim // 2, 1) * sin_b).astype(jnp.bfloat16)

    query = jnp.dot(acts, wq_ref[...], preferred_element_type=jnp.float32) + bq_ref[...].astype(jnp.float32)
    for head in range(query.shape[1] // head_dim):
        cols = slice(head * head_dim, (head + 1) * head_dim)
        q_ref[:, cols] = rotary(query[:, cols])
    weight_kv = jnp.concatenate([wk_ref[...], wv_ref[...]], axis=1)
    key_value = jnp.dot(acts, weight_kv, preferred_element_type=jnp.float32)
    k_ref[...] = rotary(key_value[:, :head_dim] + bk_ref[...].astype(jnp.float32))
    v_ref[...] = (key_value[:, head_dim:] + bv_ref[...].astype(jnp.float32)).astype(jnp.bfloat16)


def qkv_project(acts, cos_tab, sin_tab, w_q, w_k, w_v, b_q, b_k, b_v, layer, seq, rows=256):
    chunk, model = acts.shape
    head_dim = cos_tab.shape[-1]
    q_cols = w_q.shape[2]
    kv_cols = w_k.shape[2]
    row_block = lambda cols: pl.BlockSpec((rows, cols), lambda i: (i, 0))
    table = pl.BlockSpec((None, rows, head_dim), lambda i: (seq, i, 0))
    weight = lambda cols: pl.BlockSpec((None, model, cols), lambda i: (layer, 0, 0))
    bias = lambda cols: pl.BlockSpec((None, 1, cols), lambda i: (layer, 0, 0))
    return pl.pallas_call(
        qkv_kernel,
        grid=(chunk // rows,),
        in_specs=[row_block(model), table, table, weight(q_cols), weight(kv_cols), weight(kv_cols), bias(q_cols), bias(kv_cols), bias(kv_cols)],
        out_specs=[row_block(q_cols), row_block(kv_cols), row_block(kv_cols)],
        out_shape=[jax.ShapeDtypeStruct((chunk, cols), jnp.bfloat16) for cols in (q_cols, kv_cols, kv_cols)],
        compiler_params=pltpu.CompilerParams(dimension_semantics=('arbitrary',), vmem_limit_bytes=VMEM_LIMIT),
        cost_estimate=pl.CostEstimate(flops=2 * chunk * model * (q_cols + 2 * kv_cols), bytes_accessed=2 * (chunk + q_cols + 2 * kv_cols) * model, transcendentals=0),
        name='qkv_rotary',
    )(acts, cos_tab, sin_tab, w_q, w_k, w_v, b_q[:, None, :], b_k[:, None, :], b_v[:, None, :])


def attention_kernel(start_ref, q_ref, kn_ref, vn_ref, ko_ref, vo_ref, held_ref, o_ref, score_ref, *, seq, group, key_block, new_block):
    rows = q_ref.shape[0]
    head_dim = kn_ref.shape[1]
    window = ko_ref.shape[0]
    block = pl.program_id(0)
    start = start_ref[seq]
    scale = head_dim ** -0.5 * LOG2E
    query = jnp.concatenate([q_ref[:, g * head_dim:(g + 1) * head_dim] for g in range(group)], axis=0)
    token = block * rows + lax.broadcasted_iota(jnp.int32, (rows, 1), 0)
    token = jnp.concatenate([token] * group, axis=0)
    oldest = start + token - window
    top_shape = (rows * group, 128)

    def lane_max(values, top):
        for i in range(values.shape[1] // 128):
            top = jnp.maximum(top, values[:, i * 128:(i + 1) * 128])
        return top

    def lane_sum(values, total):
        for i in range(values.shape[1] // 128):
            total = total + values[:, i * 128:(i + 1) * 128]
        return total

    contract = (((1,), (1,)), ((), ()))

    def score_old(step, top):
        at = pl.multiple_of(step * key_block, key_block)
        values = lax.dot_general(query, ko_ref[pl.ds(at, key_block), :], contract, preferred_element_type=jnp.float32)
        held = held_ref[:, pl.ds(at, key_block)]
        held = jnp.where((held >= 0) & (held < start), held, HIDE)
        values = jnp.where(held > oldest, values, -jnp.inf)
        score_ref[:, pl.ds(at, key_block)] = values
        return lane_max(values, top)

    def score_new(step, top):
        at = pl.multiple_of(step * new_block, new_block)
        values = lax.dot_general(query, kn_ref[pl.ds(at, new_block), :], contract, preferred_element_type=jnp.float32)
        fresh = at + lax.broadcasted_iota(jnp.int32, (1, new_block), 1)
        values = jnp.where(fresh <= token, values, -jnp.inf)
        score_ref[:, pl.ds(pl.multiple_of(window + at, new_block), new_block)] = values
        return lane_max(values, top)

    old_steps = (jnp.minimum(start, window) + key_block - 1) // key_block
    new_steps = (block * rows + rows + new_block - 1) // new_block
    top = jnp.full(top_shape, -jnp.inf, jnp.float32)
    top = lax.fori_loop(0, old_steps, score_old, top)
    top = lax.fori_loop(0, new_steps, score_new, top)
    top = jnp.max(top, axis=1, keepdims=True)

    def weigh(at, size, value_ref, value_at, carry):
        total, mixed = carry
        weights = jnp.exp2((score_ref[:, pl.ds(at, size)] - top) * scale)
        total = lane_sum(weights, total)
        mixed = mixed + jnp.dot(weights.astype(jnp.bfloat16), value_ref[pl.ds(value_at, size), :], preferred_element_type=jnp.float32)
        return total, mixed

    def mix_old(step, carry):
        at = pl.multiple_of(step * key_block, key_block)
        return weigh(at, key_block, vo_ref, at, carry)

    def mix_new(step, carry):
        at = pl.multiple_of(step * new_block, new_block)
        return weigh(pl.multiple_of(window + at, new_block), new_block, vn_ref, at, carry)

    carry = (jnp.zeros(top_shape, jnp.float32), jnp.zeros((rows * group, head_dim), jnp.float32))
    carry = lax.fori_loop(0, old_steps, mix_old, carry)
    total, mixed = lax.fori_loop(0, new_steps, mix_new, carry)
    mixed = (mixed / jnp.sum(total, axis=1, keepdims=True)).astype(jnp.bfloat16)
    for g in range(group):
        o_ref[:, g * head_dim:(g + 1) * head_dim] = mixed[g * rows:(g + 1) * rows]


def attend(query, key_new, value_new, key_cache, value_cache, held, start_pos, layer, seq, rows=256, key_block=2048, new_block=512):
    chunk, q_cols = query.shape
    window, head_dim = key_cache.shape[2:]
    group = q_cols // head_dim
    keys = window + chunk
    whole = pl.BlockSpec((chunk, head_dim), lambda i, *_: (0, 0))
    cache = pl.BlockSpec((None, None, window, head_dim), lambda i, *_: (layer, seq, 0, 0))
    return pl.pallas_call(
        functools.partial(attention_kernel, seq=seq, group=group, key_block=key_block, new_block=new_block),
        grid_spec=pltpu.PrefetchScalarGridSpec(
            num_scalar_prefetch=1,
            grid=(chunk // rows,),
            in_specs=[pl.BlockSpec((rows, q_cols), lambda i, *_: (i, 0)), whole, whole, cache, cache, pl.BlockSpec((None, 1, window), lambda i, *_: (seq, 0, 0))],
            out_specs=pl.BlockSpec((rows, q_cols), lambda i, *_: (i, 0)),
            scratch_shapes=[pltpu.VMEM((rows * group, keys), jnp.float32)],
        ),
        out_shape=jax.ShapeDtypeStruct((chunk, q_cols), jnp.bfloat16),
        compiler_params=pltpu.CompilerParams(dimension_semantics=('arbitrary',), vmem_limit_bytes=VMEM_LIMIT),
        cost_estimate=pl.CostEstimate(flops=8 * chunk * q_cols * keys, bytes_accessed=4 * (window + chunk) * head_dim + 4 * chunk * q_cols, transcendentals=0),
        name='attend',
    )(start_pos, query, key_new, value_new, key_cache, value_cache, held)


def stream_tile(weight_ref, ring_ref, sem_ref, step, steps, layer, tiles):
    slots, _, cols = ring_ref.shape

    def copy(at):
        slot = lax.rem(at, slots)
        columns = pl.ds(pl.multiple_of(lax.rem(at, tiles) * cols, cols), cols)
        return pltpu.make_async_copy(weight_ref.at[layer, :, columns], ring_ref.at[slot], sem_ref.at[slot])

    @pl.when(step == 0)
    def _():
        for i in range(min(slots - 1, steps)):
            copy(jnp.int32(i)).start()

    @pl.when(step + slots - 1 < steps)
    def _():
        copy(step + slots - 1).start()

    copy(step).wait()
    return ring_ref[lax.rem(step, slots)]


def project_kernel(table_ref, *refs, shards, joined, layer, steps):
    acts_refs, (weight_ref, *refs), (ring_ref, sem_ref) = refs[:shards], refs[shards:-2], refs[-2:]
    weight = stream_tile(weight_ref, ring_ref, sem_ref, pl.program_id(0), steps, layer, steps)
    total = jnp.dot(jnp.concatenate([ref[...] for ref in acts_refs], axis=0), weight, preferred_element_type=jnp.float32)
    if not joined:
        refs[0][...] = total.astype(jnp.bfloat16)
    else:
        lead_ref, kept_ref, sent_ref = refs
        total = (total + lead_ref[...].astype(jnp.float32)).astype(jnp.bfloat16)
        kept_ref[...] = total[:total.shape[0] // 2]
        sent_ref[...] = total[total.shape[0] // 2:]


def project_rows(table, acts, weight, layer, lead, cols, slots=3):
    chunk, depth = acts.shape
    model = weight.shape[2]
    half = chunk // 2
    shards = table.shape[0] // 2
    part = half // shards
    first = shards if lead is None else 0
    out = lambda rows: pl.BlockSpec((rows, cols), lambda i, *_: (0, i))
    shape = lambda rows: jax.ShapeDtypeStruct((rows, model), jnp.bfloat16)
    shard = lambda at: pl.BlockSpec((part, depth), lambda i, places: (places[at], 0))
    in_specs = [shard(first + k) for k in range(shards)] + [pl.BlockSpec(memory_space=pl.ANY)]
    args = [table] + [acts] * shards + [weight]
    if lead is None:
        out_specs, out_shape = [out(half)], [shape(half)]
    else:
        in_specs.append(out(half))
        args.append(lead)
        out_specs, out_shape = [out(half // 2)] * 2, [shape(half // 2)] * 2
    return pl.pallas_call(
        functools.partial(project_kernel, shards=shards, joined=lead is not None, layer=layer, steps=model // cols),
        grid_spec=pltpu.PrefetchScalarGridSpec(
            num_scalar_prefetch=1,
            grid=(model // cols,),
            in_specs=in_specs,
            out_specs=out_specs,
            scratch_shapes=[pltpu.VMEM((slots, depth, cols), jnp.bfloat16), pltpu.SemaphoreType.DMA((slots,))],
        ),
        out_shape=out_shape,
        compiler_params=pltpu.CompilerParams(dimension_semantics=('arbitrary',), vmem_limit_bytes=VMEM_LIMIT),
        cost_estimate=pl.CostEstimate(flops=2 * half * depth * model, bytes_accessed=2 * (half * depth + depth * model + half * model), transcendentals=0),
        name='project_rows',
    )(*args)


def expand_kernel(x_ref, weight_ref, bias_ref, out_ref, ring_ref, sem_ref, *, layer, blocks, tiles):
    step = pl.program_id(0) * tiles + pl.program_id(1)
    weight = stream_tile(weight_ref, ring_ref, sem_ref, step, blocks * tiles, layer, tiles)
    lifted = jnp.dot(x_ref[...], weight, preferred_element_type=jnp.float32) + bias_ref[...].astype(jnp.float32)
    out_ref[...] = jax.nn.gelu(lifted, approximate=True).astype(jnp.bfloat16)


def expand_rows(acts, weight, bias, layer, rows=512, cols=896, slots=2):
    chunk, model = acts.shape
    width = weight.shape[2]
    blocks, tiles = chunk // rows, width // cols
    return pl.pallas_call(
        functools.partial(expand_kernel, layer=layer, blocks=blocks, tiles=tiles),
        grid=(blocks, tiles),
        in_specs=[pl.BlockSpec((rows, model), lambda i, j: (i, 0)), pl.BlockSpec(memory_space=pl.ANY), pl.BlockSpec((None, 1, cols), lambda i, j: (layer, 0, j))],
        out_specs=pl.BlockSpec((rows, cols), lambda i, j: (i, j)),
        scratch_shapes=[pltpu.VMEM((slots, model, cols), jnp.bfloat16), pltpu.SemaphoreType.DMA((slots,))],
        out_shape=jax.ShapeDtypeStruct((chunk, width), jnp.bfloat16),
        compiler_params=pltpu.CompilerParams(dimension_semantics=('arbitrary', 'arbitrary'), vmem_limit_bytes=VMEM_LIMIT),
        cost_estimate=pl.CostEstimate(flops=2 * chunk * model * width, bytes_accessed=2 * (chunk * model + blocks * model * width + chunk * width), transcendentals=0),
        name='expand',
    )(acts, weight, bias)


def cache_kernel(start_ref, ko_ref, vo_ref, kn_ref, vn_ref, kout_ref, vout_ref, ring_ref):
    window, head_dim = ko_ref.shape
    chunk = kn_ref.shape[0]
    pad = 16
    span = chunk + pad
    first = lax.rem(start_ref[pl.program_id(1)], window)
    base = pl.multiple_of((first // pad) * pad, pad)
    inner = first - base
    line = lax.broadcasted_iota(jnp.int32, (span, head_dim), 0)
    for old_ref, new_ref, out_ref in ((ko_ref, kn_ref, kout_ref), (vo_ref, vn_ref, vout_ref)):
        ring_ref[0:window] = old_ref[...]
        ring_ref[window:window + span] = old_ref[0:span]
        fresh = jnp.concatenate([new_ref[...].astype(jnp.float32), jnp.zeros((pad, head_dim), jnp.float32)], axis=0)
        fresh = pltpu.roll(fresh, inner, 0)
        kept = ring_ref[pl.ds(base, span), :].astype(jnp.float32)
        mine = (line >= inner) & (line < inner + chunk)
        ring_ref[pl.ds(base, span), :] = jnp.where(mine, fresh, kept).astype(jnp.bfloat16)
        out_ref[span:window] = ring_ref[span:window]
        wrapped = ring_ref[window:window + span].astype(jnp.float32)
        plain = ring_ref[0:span].astype(jnp.float32)
        out_ref[0:span] = jnp.where(line < first + chunk - window, wrapped, plain).astype(jnp.bfloat16)


def update_caches(start_pos, key_cache, value_cache, key_new, value_new):
    layers, seqs, window, head_dim = key_cache.shape
    chunk = key_new.shape[2]
    old = pl.BlockSpec((None, None, window, head_dim), lambda i, j, *_: (i, j, 0, 0))
    new = pl.BlockSpec((None, None, chunk, head_dim), lambda i, j, *_: (i, j, 0, 0))
    return pl.pallas_call(
        cache_kernel,
        grid_spec=pltpu.PrefetchScalarGridSpec(
            num_scalar_prefetch=1,
            grid=(layers, seqs),
            in_specs=[old, old, new, new],
            out_specs=[old, old],
            scratch_shapes=[pltpu.VMEM((window + chunk + 16, head_dim), jnp.bfloat16)],
        ),
        out_shape=[jax.ShapeDtypeStruct(key_cache.shape, jnp.bfloat16)] * 2,
        compiler_params=pltpu.CompilerParams(dimension_semantics=('arbitrary', 'arbitrary'), vmem_limit_bytes=VMEM_LIMIT),
        cost_estimate=pl.CostEstimate(flops=1 << 24, bytes_accessed=8 * layers * seqs * window * head_dim, transcendentals=0),
        name='write_caches',
    )(start_pos, key_cache, value_cache, key_new, value_new)


def solution(mesh):
    row_spec = P('dp', 'tp', None)
    cache_spec = P(None, 'dp', None, 'tp', None)
    col_spec = P(None, None, 'tp')
    bias_spec = P(None, 'tp')
    in_specs = (row_spec, P('dp'), P('dp', None, None), P('dp', None, None), cache_spec, cache_spec, P('dp', None), P(), col_spec, bias_spec, col_spec, bias_spec, col_spec, bias_spec, P(None, 'tp', None), P(), col_spec, bias_spec, P(None, 'tp', None), P())
    out_specs = (row_spec, cache_spec, cache_spec, P('dp', None))
    count = mesh.shape['tp']
    first_axis = lambda core: 1 + core
    pairs_core = [(d, d ^ 1) for d in range(count)]
    pairs_first = [(d, ((d // 2) ^ first_axis(d % 2)) * 2 + d % 2) for d in range(count)]
    pairs_second = [(d, ((d // 2) ^ (3 - first_axis(d % 2))) * 2 + d % 2) for d in range(count)]

    def device_step(tokens, start_pos, cos_tab, sin_tab, key_cache, value_cache, slot_pos, norm_params, w_q, b_q, w_k, b_k, w_v, b_v, w_o, b_o, w_up, b_up, w_down, b_down):
        num_seqs, part, _ = tokens.shape
        chunk = cos_tab.shape[1]
        head_dim = cos_tab.shape[2]
        layers = key_cache.shape[0]
        window = key_cache.shape[2]
        keys_in = key_cache.reshape(layers, num_seqs, window, head_dim)
        values_in = value_cache.reshape(layers, num_seqs, window, head_dim)
        held = slot_pos[:, None, :]
        me = lax.axis_index('tp')
        chip, core = me // 2, me % 2
        near, far = 1 + core, 2 - core
        mine = [chip ^ flip for flip in (0, far, near, 3)]
        theirs = [chip ^ flip for flip in (0, near, far, 3)]
        order = [c * 2 + core for c in mine] + [c * 2 + 1 - core for c in theirs]
        table = jnp.stack(order).astype(jnp.int32)
        norms = norm_params
        out_bias = b_o[:, None, :]
        down_bias = b_down[:, None, :]
        latest = [None]
        turn = [0]

        def item(compute, *values):
            if latest[0] is not None:
                values = lax.optimization_barrier((*values, latest[0]))[:-1]
            results = compute(*values)
            latest[0] = results[0]
            return results

        def send(value, pairs):
            return lax.ppermute(value, 'tp', pairs)

        def gather(value):
            return lax.all_gather(value, 'tp', axis=0, tiled=True)

        up_bias = b_up[:, None, :]

        def add_came(kept, came):
            return ((kept[part:].astype(jnp.float32) + came[part:].astype(jnp.float32)).astype(jnp.bfloat16),)

        def scatter_sum(lead, acts, weight, layer, cols):
            lead = send(lead, pairs_core)
            yield
            kept, sent = item(lambda lead: project_rows(table, acts, weight, layer, lead, cols), lead)
            came = send(sent, pairs_first)
            yield
            onward, = item(add_came, kept, came)
            last = send(onward, pairs_second)
            yield
            return kept, came, last

        def attention(gathered, layer, seq):
            query, key_new, value_new = qkv_project(gathered, cos_tab, sin_tab, w_q, w_k, w_v, b_q, b_k, b_v, layer, seq)
            fresh_keys[layer][seq] = key_new
            fresh_values[layer][seq] = value_new
            mixed = attend(query, key_new, value_new, keys_in, values_in, held, start_pos, layer, seq)
            lead, = project_rows(table, mixed, w_o, layer, None, 2048)
            return lead, mixed

        def expand(gathered, layer):
            active = expand_rows(gathered, w_up, up_bias, layer)
            lead, = project_rows(table, active, w_down, layer, None, 1024)
            return lead, active

        def finish(middle, kept, came, last):
            summed = kept[:part].astype(jnp.float32) + came[:part].astype(jnp.float32) + last.astype(jnp.float32)
            return ((middle.astype(jnp.float32) + summed + b_down[layers - 1].astype(jnp.float32)).astype(jnp.bfloat16),)

        def join(base, *terms, bias, layer, which):
            middle, normed = normalize(base, seq_of[0], terms, (bias, layer), norms, layer + which // 4, which % 4)
            return normed, middle

        seq_of = [0]
        fresh_keys = [[None] * num_seqs for _ in range(layers)]
        fresh_values = [[None] * num_seqs for _ in range(layers)]
        hidden_out = [None] * num_seqs

        def stream(seq):
            base = tokens
            normed, = item(lambda: normalize(base, seq, None, None, norms, 0, 0))
            for layer in range(layers):
                gathered = gather(normed)
                yield
                lead, own = item(functools.partial(attention, layer=layer, seq=seq), gathered)
                terms = yield from scatter_sum(lead, own, w_o, layer, 2048)
                seq_of[0] = seq
                normed, middle = item(lambda *terms: join(base, *terms, bias=out_bias, layer=layer, which=2), *terms)
                gathered = gather(normed)
                yield
                lead, own = item(functools.partial(expand, layer=layer), gathered)
                terms = yield from scatter_sum(lead, own, w_down, layer, 1024)
                if layer + 1 < layers:
                    seq_of[0] = seq
                    normed, base = item(lambda *terms: join(middle, *terms, bias=down_bias, layer=layer, which=4), *terms)
                else:
                    hidden_out[seq], = item(finish, middle, *terms)
            yield

        streams = [stream(seq) for seq in range(num_seqs)]
        for step, seq in enumerate(TURNS):
            turn[0] = step
            next(streams[seq])
        fresh_keys = [jnp.stack(k) for k in fresh_keys]
        fresh_values = [jnp.stack(v) for v in fresh_values]
        key_out, value_out = update_caches(start_pos, keys_in, values_in, jnp.stack(fresh_keys), jnp.stack(fresh_values))
        first_slot = start_pos % window
        offset = (jnp.arange(window)[None, :] - first_slot[:, None]) % window
        pos_out = jnp.where(offset < chunk, start_pos[:, None] + offset, slot_pos)
        return jnp.stack(hidden_out), key_out.reshape(key_cache.shape), value_out.reshape(value_cache.shape), pos_out

    return jax.shard_map(device_step, mesh=mesh, in_specs=in_specs, out_specs=out_specs, check_vma=False)
```

```python
import functools

import jax
import jax.numpy as jnp
from jax import lax
from jax.experimental import pallas as pl
from jax.experimental.pallas import tpu as pltpu
from jax.sharding import PartitionSpec as P


NORM_EPS = 1e-5
LOG2E = 1.4426950408889634
HIDE = -(1 << 30)
VMEM_LIMIT = 60 << 20
TURNS = [int(c) for c in '212021212010120201212010120201212010120201102100120']


def norm_kernel(*refs, joined, which):
    if joined:
        base_ref, pair_ref, came_ref, last_ref, bias_ref, scale_ref, sum_ref, norm_ref = refs
        summed = pair_ref[...].astype(jnp.float32) + came_ref[...].astype(jnp.float32) + last_ref[...].astype(jnp.float32)
        kept = (base_ref[...].astype(jnp.float32) + summed + bias_ref[...].astype(jnp.float32)).astype(jnp.bfloat16)
        sum_ref[...] = kept
    else:
        base_ref, scale_ref, norm_ref = refs
        kept = base_ref[...]
    values = kept.astype(jnp.float32)
    centered = values - jnp.mean(values, axis=-1, keepdims=True)
    variance = jnp.mean(centered * centered, axis=-1, keepdims=True)
    scaled = centered * lax.rsqrt(variance + NORM_EPS)
    norm_ref[...] = (scaled * scale_ref[which:which + 1, :].astype(jnp.float32) + scale_ref[which + 1:which + 2, :].astype(jnp.float32)).astype(jnp.bfloat16)


def normalize(base, seq, terms, bias, norms, layer, which, rows=64):
    part, model = base.shape[-2:]
    line = pl.BlockSpec((rows, model), lambda i: (i, 0))
    first = line if base.ndim == 2 else pl.BlockSpec((None, rows, model), lambda i: (seq, i, 0))
    vector = lambda at: pl.BlockSpec((None, 1, model), lambda i: (at, 0, 0))
    scale_specs = [pl.BlockSpec((None, norms.shape[1], model), lambda i: (layer, 0, 0))]
    scales = [norms]
    whole = jax.ShapeDtypeStruct((part, model), jnp.bfloat16)
    if terms is None:
        specs, args, outs = [first], [base], [whole]
    else:
        bias, bias_at = bias
        specs, args, outs = [first, line, line, line, vector(bias_at)], [base, *terms, bias], [whole, whole]
    return pl.pallas_call(
        functools.partial(norm_kernel, joined=terms is not None, which=which),
        grid=(part // rows,),
        in_specs=specs + scale_specs,
        out_specs=[line] * len(outs),
        out_shape=outs,
        compiler_params=pltpu.CompilerParams(dimension_semantics=('arbitrary',), vmem_limit_bytes=VMEM_LIMIT),
        cost_estimate=pl.CostEstimate(flops=8 * part * model, bytes_accessed=2 * (len(args) + len(outs)) * part * model, transcendentals=0),
        name='norm',
    )(*args, *scales)


def qkv_kernel(x_ref, cos_ref, sin_ref, wq_ref, wk_ref, wv_ref, bq_ref, bk_ref, bv_ref, q_ref, k_ref, v_ref):
    head_dim = cos_ref.shape[-1]
    acts = x_ref[...]
    cos_b = cos_ref[...]
    lane = lax.broadcasted_iota(jnp.int32, cos_b.shape, 1)
    sin_b = jnp.where(lane < head_dim // 2, -sin_ref[...], sin_ref[...])

    def rotary(values):
        return (values * cos_b + pltpu.roll(values, head_dim // 2, 1) * sin_b).astype(jnp.bfloat16)

    query = jnp.dot(acts, wq_ref[...], preferred_element_type=jnp.float32) + bq_ref[...].astype(jnp.float32)
    for head in range(query.shape[1] // head_dim):
        cols = slice(head * head_dim, (head + 1) * head_dim)
        q_ref[:, cols] = rotary(query[:, cols])
    weight_kv = jnp.concatenate([wk_ref[...], wv_ref[...]], axis=1)
    key_value = jnp.dot(acts, weight_kv, preferred_element_type=jnp.float32)
    k_ref[...] = rotary(key_value[:, :head_dim] + bk_ref[...].astype(jnp.float32))
    v_ref[...] = (key_value[:, head_dim:] + bv_ref[...].astype(jnp.float32)).astype(jnp.bfloat16)


def qkv_project(acts, cos_tab, sin_tab, w_q, w_k, w_v, b_q, b_k, b_v, layer, seq, rows=256):
    chunk, model = acts.shape
    head_dim = cos_tab.shape[-1]
    q_cols = w_q.shape[2]
    kv_cols = w_k.shape[2]
    row_block = lambda cols: pl.BlockSpec((rows, cols), lambda i: (i, 0))
    table = pl.BlockSpec((None, rows, head_dim), lambda i: (seq, i, 0))
    weight = lambda cols: pl.BlockSpec((None, model, cols), lambda i: (layer, 0, 0))
    bias = lambda cols: pl.BlockSpec((None, 1, cols), lambda i: (layer, 0, 0))
    return pl.pallas_call(
        qkv_kernel,
        grid=(chunk // rows,),
        in_specs=[row_block(model), table, table, weight(q_cols), weight(kv_cols), weight(kv_cols), bias(q_cols), bias(kv_cols), bias(kv_cols)],
        out_specs=[row_block(q_cols), row_block(kv_cols), row_block(kv_cols)],
        out_shape=[jax.ShapeDtypeStruct((chunk, cols), jnp.bfloat16) for cols in (q_cols, kv_cols, kv_cols)],
        compiler_params=pltpu.CompilerParams(dimension_semantics=('arbitrary',), vmem_limit_bytes=VMEM_LIMIT),
        cost_estimate=pl.CostEstimate(flops=2 * chunk * model * (q_cols + 2 * kv_cols), bytes_accessed=2 * (chunk + q_cols + 2 * kv_cols) * model, transcendentals=0),
        name='qkv_rotary',
    )(acts, cos_tab, sin_tab, w_q, w_k, w_v, b_q[:, None, :], b_k[:, None, :], b_v[:, None, :])


def attention_kernel(start_ref, q_ref, kn_ref, vn_ref, ko_ref, vo_ref, held_ref, o_ref, score_ref, peak_ref, top_ref, total_ref, mixed_ref, *, seq, group, key_block, new_block):
    rows = q_ref.shape[0]
    head_dim = kn_ref.shape[1]
    window = ko_ref.shape[0]
    block = pl.program_id(0)
    start = start_ref[seq]
    scale = head_dim ** -0.5 * LOG2E
    query = jnp.concatenate([q_ref[:, g * head_dim:(g + 1) * head_dim] for g in range(group)], axis=0)
    token = block * rows + lax.broadcasted_iota(jnp.int32, (rows, 1), 0)
    token = jnp.concatenate([token] * group, axis=0)
    oldest = start + token - window
    half = rows * group // 2
    spans = [slice(i * half, (i + 1) * half) for i in range(2)]

    def lane_max(values, top):
        for i in range(values.shape[1] // 128):
            top = jnp.maximum(top, values[:, i * 128:(i + 1) * 128])
        return top

    def lane_sum(values, total):
        for i in range(values.shape[1] // 128):
            total = total + values[:, i * 128:(i + 1) * 128]
        return total

    contract = (((1,), (1,)), ((), ()))

    def score_old(step, top):
        at = pl.multiple_of(step * key_block, key_block)
        held = held_ref[:, pl.ds(at, key_block)]
        held = jnp.where((held >= 0) & (held < start), held, HIDE)
        keys = ko_ref[pl.ds(at, key_block), :]
        for span in spans:
            values = lax.dot_general(query[span], keys, contract, preferred_element_type=jnp.float32)
            values = jnp.where(held > oldest[span], values * scale, -jnp.inf)
            score_ref[span, pl.ds(at, key_block)] = values
            peak_ref[span, :] = lane_max(values, peak_ref[span, :])
        return top

    def score_new(step, top):
        at = pl.multiple_of(step * new_block, new_block)
        fresh = at + lax.broadcasted_iota(jnp.int32, (1, new_block), 1)
        keys = kn_ref[pl.ds(at, new_block), :]
        for span in spans:
            values = lax.dot_general(query[span], keys, contract, preferred_element_type=jnp.float32)
            values = jnp.where(fresh <= token[span], values * scale, -jnp.inf)
            score_ref[span, pl.ds(pl.multiple_of(window + at, new_block), new_block)] = values
            peak_ref[span, :] = lane_max(values, peak_ref[span, :])
        return top

    old_steps = (jnp.minimum(start, window) + key_block - 1) // key_block
    new_steps = (block * rows + rows + new_block - 1) // new_block
    peak_ref[...] = jnp.full_like(peak_ref, -jnp.inf)
    lax.fori_loop(0, old_steps, score_old, 0)
    lax.fori_loop(0, new_steps, score_new, 0)
    top_ref[...] = jnp.max(peak_ref[...], axis=1, keepdims=True)
    total_ref[...] = jnp.zeros_like(total_ref)
    mixed_ref[...] = jnp.zeros_like(mixed_ref)

    def weigh(at, size, value_ref, value_at, carry):
        value = value_ref[pl.ds(value_at, size), :]
        for span in spans:
            weights = jnp.exp2(score_ref[span, pl.ds(at, size)] - top_ref[span, :])
            total_ref[span, :] = lane_sum(weights, total_ref[span, :])
            mixed_ref[span, :] += jnp.dot(weights.astype(jnp.bfloat16), value, preferred_element_type=jnp.float32)
        return carry

    def mix_old(step, carry):
        at = pl.multiple_of(step * key_block, key_block)
        return weigh(at, key_block, vo_ref, at, carry)

    def mix_new(step, carry):
        at = pl.multiple_of(step * new_block, new_block)
        return weigh(pl.multiple_of(window + at, new_block), new_block, vn_ref, at, carry)

    lax.fori_loop(0, old_steps, mix_old, 0)
    lax.fori_loop(0, new_steps, mix_new, 0)
    mixed = (mixed_ref[...] / jnp.sum(total_ref[...], axis=1, keepdims=True)).astype(jnp.bfloat16)
    for g in range(group):
        o_ref[:, g * head_dim:(g + 1) * head_dim] = mixed[g * rows:(g + 1) * rows]


def attend(query, key_new, value_new, key_cache, value_cache, held, start_pos, layer, seq, rows=256, key_block=2048, new_block=512):
    chunk, q_cols = query.shape
    window, head_dim = key_cache.shape[2:]
    group = q_cols // head_dim
    keys = window + chunk
    whole = pl.BlockSpec((chunk, head_dim), lambda i, *_: (0, 0))
    cache = pl.BlockSpec((None, None, window, head_dim), lambda i, *_: (layer, seq, 0, 0))
    return pl.pallas_call(
        functools.partial(attention_kernel, seq=seq, group=group, key_block=key_block, new_block=new_block),
        grid_spec=pltpu.PrefetchScalarGridSpec(
            num_scalar_prefetch=1,
            grid=(chunk // rows,),
            in_specs=[pl.BlockSpec((rows, q_cols), lambda i, *_: (i, 0)), whole, whole, cache, cache, pl.BlockSpec((None, 1, window), lambda i, *_: (seq, 0, 0))],
            out_specs=pl.BlockSpec((rows, q_cols), lambda i, *_: (i, 0)),
            scratch_shapes=[pltpu.VMEM((rows * group, keys), jnp.float32), pltpu.VMEM((rows * group, 128), jnp.float32), pltpu.VMEM((rows * group, 1), jnp.float32), pltpu.VMEM((rows * group, 128), jnp.float32), pltpu.VMEM((rows * group, head_dim), jnp.float32)],
        ),
        out_shape=jax.ShapeDtypeStruct((chunk, q_cols), jnp.bfloat16),
        compiler_params=pltpu.CompilerParams(dimension_semantics=('arbitrary',), vmem_limit_bytes=VMEM_LIMIT),
        cost_estimate=pl.CostEstimate(flops=8 * chunk * q_cols * keys, bytes_accessed=4 * (window + chunk) * head_dim + 4 * chunk * q_cols, transcendentals=0),
        name='attend',
    )(start_pos, query, key_new, value_new, key_cache, value_cache, held)


def stream_tile(weight_ref, ring_ref, sem_ref, step, steps, layer, tiles):
    slots, _, cols = ring_ref.shape

    def copy(at):
        slot = lax.rem(at, slots)
        columns = pl.ds(pl.multiple_of(lax.rem(at, tiles) * cols, cols), cols)
        return pltpu.make_async_copy(weight_ref.at[layer, :, columns], ring_ref.at[slot], sem_ref.at[slot])

    @pl.when(step == 0)
    def _():
        for i in range(min(slots - 1, steps)):
            copy(jnp.int32(i)).start()

    @pl.when(step + slots - 1 < steps)
    def _():
        copy(step + slots - 1).start()

    copy(step).wait()
    return ring_ref[lax.rem(step, slots)]


def project_kernel(table_ref, *refs, shards, joined, layer, steps):
    acts_refs, (weight_ref, *refs), (ring_ref, sem_ref) = refs[:shards], refs[shards:-2], refs[-2:]
    weight = stream_tile(weight_ref, ring_ref, sem_ref, pl.program_id(0), steps, layer, steps)
    total = jnp.dot(jnp.concatenate([ref[...] for ref in acts_refs], axis=0), weight, preferred_element_type=jnp.float32)
    if not joined:
        refs[0][...] = total.astype(jnp.bfloat16)
    else:
        lead_ref, kept_ref, sent_ref = refs
        total = (total + lead_ref[...].astype(jnp.float32)).astype(jnp.bfloat16)
        kept_ref[...] = total[:total.shape[0] // 2]
        sent_ref[...] = total[total.shape[0] // 2:]


def project_rows(table, acts, part, weight, layer, lead, cols, slots=4):
    depth, model = weight.shape[1:]
    shards = table.shape[0] // 2
    picked = acts.shape[0] // part == shards
    half = part * shards
    first = 0 if picked or lead is not None else shards
    out = lambda rows: pl.BlockSpec((rows, cols), lambda i, *_: (0, i))
    shape = lambda rows: jax.ShapeDtypeStruct((rows, model), jnp.bfloat16)
    shard = lambda at: pl.BlockSpec((part, depth), lambda i, places: (at if picked else places[at], 0))
    in_specs = [shard(first + k) for k in range(shards)] + [pl.BlockSpec(memory_space=pl.ANY)]
    args = [table] + [acts] * shards + [weight]
    if lead is None:
        out_specs, out_shape = [out(half)], [shape(half)]
    else:
        in_specs.append(out(half))
        args.append(lead)
        out_specs, out_shape = [out(half // 2)] * 2, [shape(half // 2)] * 2
    return pl.pallas_call(
        functools.partial(project_kernel, shards=shards, joined=lead is not None, layer=layer, steps=model // cols),
        grid_spec=pltpu.PrefetchScalarGridSpec(
            num_scalar_prefetch=1,
            grid=(model // cols,),
            in_specs=in_specs,
            out_specs=out_specs,
            scratch_shapes=[pltpu.VMEM((slots, depth, cols), jnp.bfloat16), pltpu.SemaphoreType.DMA((slots,))],
        ),
        out_shape=out_shape,
        compiler_params=pltpu.CompilerParams(dimension_semantics=('arbitrary',), vmem_limit_bytes=VMEM_LIMIT),
        cost_estimate=pl.CostEstimate(flops=2 * half * depth * model, bytes_accessed=2 * (half * depth + depth * model + half * model), transcendentals=0),
        name='project_rows',
    )(*args)


def expand_kernel(table_ref, *refs, shards, layer, tiles):
    x_refs, (weight_ref, bias_ref, out_ref, ring_ref, sem_ref) = refs[:shards], refs[shards:]
    weight = stream_tile(weight_ref, ring_ref, sem_ref, pl.program_id(0), tiles, layer, tiles)
    acts = jnp.concatenate([ref[...] for ref in x_refs], axis=0)
    lifted = jnp.dot(acts, weight, preferred_element_type=jnp.float32) + bias_ref[...].astype(jnp.float32)
    out_ref[...] = jax.nn.gelu(lifted, approximate=True).astype(jnp.bfloat16)


def expand_rows(table, acts, weight, bias, layer, first, cols=256, slots=4):
    chunk, model = acts.shape
    width = weight.shape[2]
    tiles = width // cols
    shards = table.shape[0] // 2
    part = chunk // table.shape[0]
    rows = part * shards
    shard = lambda at: pl.BlockSpec((part, model), lambda i, places: (places[at], 0))
    return pl.pallas_call(
        functools.partial(expand_kernel, shards=shards, layer=layer, tiles=tiles),
        grid_spec=pltpu.PrefetchScalarGridSpec(
            num_scalar_prefetch=1,
            grid=(tiles,),
            in_specs=[shard(first + k) for k in range(shards)] + [pl.BlockSpec(memory_space=pl.ANY), pl.BlockSpec((None, 1, cols), lambda i, *_: (layer, 0, i))],
            out_specs=pl.BlockSpec((rows, cols), lambda i, *_: (0, i)),
            scratch_shapes=[pltpu.VMEM((slots, model, cols), jnp.bfloat16), pltpu.SemaphoreType.DMA((slots,))],
        ),
        out_shape=jax.ShapeDtypeStruct((rows, width), jnp.bfloat16),
        compiler_params=pltpu.CompilerParams(dimension_semantics=('arbitrary',), vmem_limit_bytes=VMEM_LIMIT),
        cost_estimate=pl.CostEstimate(flops=2 * rows * model * width, bytes_accessed=2 * (rows * model + model * width + rows * width), transcendentals=0),
        name='expand',
    )(table, *[acts] * shards, weight, bias)


def cache_kernel(start_ref, ko_ref, vo_ref, kn_ref, vn_ref, kout_ref, vout_ref, ring_ref):
    window, head_dim = ko_ref.shape
    chunk = kn_ref.shape[0]
    pad = 16
    span = chunk + pad
    first = lax.rem(start_ref[pl.program_id(1)], window)
    base = pl.multiple_of((first // pad) * pad, pad)
    inner = first - base
    line = lax.broadcasted_iota(jnp.int32, (span, head_dim), 0)
    for old_ref, new_ref, out_ref in ((ko_ref, kn_ref, kout_ref), (vo_ref, vn_ref, vout_ref)):
        ring_ref[0:window] = old_ref[...]
        ring_ref[window:window + span] = old_ref[0:span]
        fresh = jnp.concatenate([new_ref[...].astype(jnp.float32), jnp.zeros((pad, head_dim), jnp.float32)], axis=0)
        fresh = pltpu.roll(fresh, inner, 0)
        kept = ring_ref[pl.ds(base, span), :].astype(jnp.float32)
        mine = (line >= inner) & (line < inner + chunk)
        ring_ref[pl.ds(base, span), :] = jnp.where(mine, fresh, kept).astype(jnp.bfloat16)
        out_ref[span:window] = ring_ref[span:window]
        wrapped = ring_ref[window:window + span].astype(jnp.float32)
        plain = ring_ref[0:span].astype(jnp.float32)
        out_ref[0:span] = jnp.where(line < first + chunk - window, wrapped, plain).astype(jnp.bfloat16)


def update_caches(start_pos, key_cache, value_cache, key_new, value_new):
    layers, seqs, window, head_dim = key_cache.shape
    chunk = key_new.shape[2]
    old = pl.BlockSpec((None, None, window, head_dim), lambda i, j, *_: (i, j, 0, 0))
    new = pl.BlockSpec((None, None, chunk, head_dim), lambda i, j, *_: (i, j, 0, 0))
    return pl.pallas_call(
        cache_kernel,
        grid_spec=pltpu.PrefetchScalarGridSpec(
            num_scalar_prefetch=1,
            grid=(layers, seqs),
            in_specs=[old, old, new, new],
            out_specs=[old, old],
            scratch_shapes=[pltpu.VMEM((window + chunk + 16, head_dim), jnp.bfloat16)],
        ),
        out_shape=[jax.ShapeDtypeStruct(key_cache.shape, jnp.bfloat16)] * 2,
        compiler_params=pltpu.CompilerParams(dimension_semantics=('arbitrary', 'arbitrary'), vmem_limit_bytes=VMEM_LIMIT),
        cost_estimate=pl.CostEstimate(flops=1 << 24, bytes_accessed=8 * layers * seqs * window * head_dim, transcendentals=0),
        name='write_caches',
    )(start_pos, key_cache, value_cache, key_new, value_new)


def solution(mesh):
    row_spec = P('dp', 'tp', None)
    cache_spec = P(None, 'dp', None, 'tp', None)
    col_spec = P(None, None, 'tp')
    bias_spec = P(None, 'tp')
    in_specs = (row_spec, P('dp'), P('dp', None, None), P('dp', None, None), cache_spec, cache_spec, P('dp', None), P(), col_spec, bias_spec, col_spec, bias_spec, col_spec, bias_spec, P(None, 'tp', None), P(), col_spec, bias_spec, P(None, 'tp', None), P())
    out_specs = (row_spec, cache_spec, cache_spec, P('dp', None))
    count = mesh.shape['tp']
    first_axis = lambda core: 1 + core
    pairs_core = [(d, d ^ 1) for d in range(count)]
    pairs_first = [(d, ((d // 2) ^ first_axis(d % 2)) * 2 + d % 2) for d in range(count)]
    pairs_second = [(d, ((d // 2) ^ (3 - first_axis(d % 2))) * 2 + d % 2) for d in range(count)]

    def device_step(tokens, start_pos, cos_tab, sin_tab, key_cache, value_cache, slot_pos, norm_params, w_q, b_q, w_k, b_k, w_v, b_v, w_o, b_o, w_up, b_up, w_down, b_down):
        num_seqs, part, _ = tokens.shape
        chunk = cos_tab.shape[1]
        head_dim = cos_tab.shape[2]
        layers = key_cache.shape[0]
        window = key_cache.shape[2]
        keys_in = key_cache.reshape(layers, num_seqs, window, head_dim)
        values_in = value_cache.reshape(layers, num_seqs, window, head_dim)
        held = slot_pos[:, None, :]
        me = lax.axis_index('tp')
        chip, core = me // 2, me % 2
        near, far = 1 + core, 2 - core
        mine = [chip ^ flip for flip in (0, far, near, 3)]
        theirs = [chip ^ flip for flip in (0, near, far, 3)]
        order = [c * 2 + core for c in mine] + [c * 2 + 1 - core for c in theirs]
        table = jnp.stack(order).astype(jnp.int32)
        norms = norm_params
        out_bias = b_o[:, None, :]
        down_bias = b_down[:, None, :]
        latest = [None]
        turn = [0]

        def item(compute, *values):
            if latest[0] is not None:
                values = lax.optimization_barrier((*values, latest[0]))[:-1]
            results = compute(*values)
            latest[0] = results[0]
            return results

        def send(value, pairs):
            return lax.ppermute(value, 'tp', pairs)

        def gather(value):
            return lax.all_gather(value, 'tp', axis=0, tiled=True)

        up_bias = b_up[:, None, :]

        def add_came(kept, came):
            return ((kept[part:].astype(jnp.float32) + came[part:].astype(jnp.float32)).astype(jnp.bfloat16),)

        def scatter_sum(lead, acts, make_acts, weight, layer, cols):
            lead = send(lead, pairs_core)
            yield
            kept, sent = item(lambda acts: project_rows(table, make_acts(acts), part, weight, layer, lead, cols), acts)
            came = send(sent, pairs_first)
            yield
            onward, = item(add_came, kept, came)
            last = send(onward, pairs_second)
            yield
            return kept, came, last

        def attention(gathered, layer, seq):
            query, key_new, value_new = qkv_project(gathered, cos_tab, sin_tab, w_q, w_k, w_v, b_q, b_k, b_v, layer, seq)
            fresh_keys[layer][seq] = key_new
            fresh_values[layer][seq] = value_new
            mixed = attend(query, key_new, value_new, keys_in, values_in, held, start_pos, layer, seq)
            lead, = project_rows(table, mixed, part, w_o, layer, None, 1024)
            return lead, mixed

        def expand(gathered, layer):
            active = expand_rows(table, gathered, w_up, up_bias, layer, count // 2)
            lead, = project_rows(table, active, part, w_down, layer, None, 512)
            return lead, gathered

        def finish(middle, kept, came, last):
            summed = kept[:part].astype(jnp.float32) + came[:part].astype(jnp.float32) + last.astype(jnp.float32)
            return ((middle.astype(jnp.float32) + summed + b_down[layers - 1].astype(jnp.float32)).astype(jnp.bfloat16),)

        def join(base, *terms, bias, layer, which):
            middle, normed = normalize(base, seq_of[0], terms, (bias, layer), norms, layer + which // 4, which % 4)
            return normed, middle

        seq_of = [0]
        fresh_keys = [[None] * num_seqs for _ in range(layers)]
        fresh_values = [[None] * num_seqs for _ in range(layers)]
        hidden_out = [None] * num_seqs

        def stream(seq):
            base = tokens
            normed, = item(lambda: normalize(base, seq, None, None, norms, 0, 0))
            for layer in range(layers):
                gathered = gather(normed)
                yield
                lead, own = item(functools.partial(attention, layer=layer, seq=seq), gathered)
                terms = yield from scatter_sum(lead, own, lambda mixed: mixed, w_o, layer, 1024)
                seq_of[0] = seq
                normed, middle = item(lambda *terms: join(base, *terms, bias=out_bias, layer=layer, which=2), *terms)
                gathered = gather(normed)
                yield
                lead, own = item(functools.partial(expand, layer=layer), gathered)
                terms = yield from scatter_sum(lead, own, lambda acts: expand_rows(table, acts, w_up, up_bias, layer, 0), w_down, layer, 512)
                if layer + 1 < layers:
                    seq_of[0] = seq
                    normed, base = item(lambda *terms: join(middle, *terms, bias=down_bias, layer=layer, which=4), *terms)
                else:
                    hidden_out[seq], = item(finish, middle, *terms)
            yield

        streams = [stream(seq) for seq in range(num_seqs)]
        for step, seq in enumerate(TURNS):
            turn[0] = step
            next(streams[seq])
        fresh_keys = [jnp.stack(k) for k in fresh_keys]
        fresh_values = [jnp.stack(v) for v in fresh_values]
        key_out, value_out = update_caches(start_pos, keys_in, values_in, jnp.stack(fresh_keys), jnp.stack(fresh_values))
        first_slot = start_pos % window
        offset = (jnp.arange(window)[None, :] - first_slot[:, None]) % window
        pos_out = jnp.where(offset < chunk, start_pos[:, None] + offset, slot_pos)
        return jnp.stack(hidden_out), key_out.reshape(key_cache.shape), value_out.reshape(value_cache.shape), pos_out

    return jax.shard_map(device_step, mesh=mesh, in_specs=in_specs, out_specs=out_specs, check_vma=False)
```

```python
import functools

import jax
import jax.numpy as jnp
from jax import lax
from jax.experimental import pallas as pl
from jax.experimental.pallas import tpu as pltpu
from jax.sharding import PartitionSpec as P


NORM_EPS = 1e-5
LOG2E = 1.4426950408889634
HIDE = -(1 << 30)
VMEM_LIMIT = 60 << 20
TURNS = [int(c) for c in '212021212010120201212010120201212010120201102100120']


def norm_kernel(*refs, joined, which):
    if joined:
        base_ref, pair_ref, came_ref, last_ref, bias_ref, scale_ref, sum_ref, norm_ref = refs
        summed = pair_ref[...].astype(jnp.float32) + came_ref[...].astype(jnp.float32) + last_ref[...].astype(jnp.float32)
        kept = (base_ref[...].astype(jnp.float32) + summed + bias_ref[...].astype(jnp.float32)).astype(jnp.bfloat16)
        sum_ref[...] = kept
    else:
        base_ref, scale_ref, norm_ref = refs
        kept = base_ref[...]
    values = kept.astype(jnp.float32)
    centered = values - jnp.mean(values, axis=-1, keepdims=True)
    variance = jnp.mean(centered * centered, axis=-1, keepdims=True)
    scaled = centered * lax.rsqrt(variance + NORM_EPS)
    norm_ref[...] = (scaled * scale_ref[which:which + 1, :].astype(jnp.float32) + scale_ref[which + 1:which + 2, :].astype(jnp.float32)).astype(jnp.bfloat16)


def normalize(base, seq, terms, bias, norms, layer, which, rows=64):
    part, model = base.shape[-2:]
    line = pl.BlockSpec((rows, model), lambda i: (i, 0))
    first = line if base.ndim == 2 else pl.BlockSpec((None, rows, model), lambda i: (seq, i, 0))
    vector = lambda at: pl.BlockSpec((None, 1, model), lambda i: (at, 0, 0))
    scale_specs = [pl.BlockSpec((None, norms.shape[1], model), lambda i: (layer, 0, 0))]
    scales = [norms]
    whole = jax.ShapeDtypeStruct((part, model), jnp.bfloat16)
    if terms is None:
        specs, args, outs = [first], [base], [whole]
    else:
        bias, bias_at = bias
        specs, args, outs = [first, line, line, line, vector(bias_at)], [base, *terms, bias], [whole, whole]
    return pl.pallas_call(
        functools.partial(norm_kernel, joined=terms is not None, which=which),
        grid=(part // rows,),
        in_specs=specs + scale_specs,
        out_specs=[line] * len(outs),
        out_shape=outs,
        compiler_params=pltpu.CompilerParams(dimension_semantics=('arbitrary',), vmem_limit_bytes=VMEM_LIMIT),
        cost_estimate=pl.CostEstimate(flops=8 * part * model, bytes_accessed=2 * (len(args) + len(outs)) * part * model, transcendentals=0),
        name='norm',
    )(*args, *scales)


def qkv_kernel(x_ref, cos_ref, sin_ref, wq_ref, wk_ref, wv_ref, bq_ref, bk_ref, bv_ref, q_ref, k_ref, v_ref):
    head_dim = cos_ref.shape[-1]
    acts = x_ref[...]
    cos_b = cos_ref[...]
    lane = lax.broadcasted_iota(jnp.int32, cos_b.shape, 1)
    sin_b = jnp.where(lane < head_dim // 2, -sin_ref[...], sin_ref[...])

    def rotary(values):
        return (values * cos_b + pltpu.roll(values, head_dim // 2, 1) * sin_b).astype(jnp.bfloat16)

    query = jnp.dot(acts, wq_ref[...], preferred_element_type=jnp.float32) + bq_ref[...].astype(jnp.float32)
    for head in range(query.shape[1] // head_dim):
        cols = slice(head * head_dim, (head + 1) * head_dim)
        q_ref[:, cols] = rotary(query[:, cols])
    weight_kv = jnp.concatenate([wk_ref[...], wv_ref[...]], axis=1)
    key_value = jnp.dot(acts, weight_kv, preferred_element_type=jnp.float32)
    k_ref[...] = rotary(key_value[:, :head_dim] + bk_ref[...].astype(jnp.float32))
    v_ref[...] = (key_value[:, head_dim:] + bv_ref[...].astype(jnp.float32)).astype(jnp.bfloat16)


def qkv_project(acts, cos_tab, sin_tab, w_q, w_k, w_v, b_q, b_k, b_v, layer, seq, rows=256):
    chunk, model = acts.shape
    head_dim = cos_tab.shape[-1]
    q_cols = w_q.shape[2]
    kv_cols = w_k.shape[2]
    row_block = lambda cols: pl.BlockSpec((rows, cols), lambda i: (i, 0))
    table = pl.BlockSpec((None, rows, head_dim), lambda i: (seq, i, 0))
    weight = lambda cols: pl.BlockSpec((None, model, cols), lambda i: (layer, 0, 0))
    bias = lambda cols: pl.BlockSpec((None, 1, cols), lambda i: (layer, 0, 0))
    return pl.pallas_call(
        qkv_kernel,
        grid=(chunk // rows,),
        in_specs=[row_block(model), table, table, weight(q_cols), weight(kv_cols), weight(kv_cols), bias(q_cols), bias(kv_cols), bias(kv_cols)],
        out_specs=[row_block(q_cols), row_block(kv_cols), row_block(kv_cols)],
        out_shape=[jax.ShapeDtypeStruct((chunk, cols), jnp.bfloat16) for cols in (q_cols, kv_cols, kv_cols)],
        compiler_params=pltpu.CompilerParams(dimension_semantics=('arbitrary',), vmem_limit_bytes=VMEM_LIMIT),
        cost_estimate=pl.CostEstimate(flops=2 * chunk * model * (q_cols + 2 * kv_cols), bytes_accessed=2 * (chunk + q_cols + 2 * kv_cols) * model, transcendentals=0),
        name='qkv_rotary',
    )(acts, cos_tab, sin_tab, w_q, w_k, w_v, b_q[:, None, :], b_k[:, None, :], b_v[:, None, :])


def attention_kernel(start_ref, table_ref, q_ref, kn_ref, vn_ref, ko_ref, vo_ref, held_ref, weight_ref, o_ref, lead_ref, score_ref, peak_ref, top_ref, total_ref, mixed_ref, all_ref, tile_ref, stage_ref, tile_sem, stage_sem, *, layer, seq, group, key_block, new_block):
    rows = q_ref.shape[0]
    head_dim = kn_ref.shape[1]
    window = ko_ref.shape[0]
    block = pl.program_id(0)
    start = start_ref[seq]
    scale = head_dim ** -0.5 * LOG2E
    query = jnp.concatenate([q_ref[:, g * head_dim:(g + 1) * head_dim] for g in range(group)], axis=0)
    token = block * rows + lax.broadcasted_iota(jnp.int32, (rows, 1), 0)
    token = jnp.concatenate([token] * group, axis=0)
    oldest = start + token - window
    half = rows * group // 2
    spans = [slice(i * half, (i + 1) * half) for i in range(2)]

    def lane_max(values, top):
        for i in range(values.shape[1] // 128):
            top = jnp.maximum(top, values[:, i * 128:(i + 1) * 128])
        return top

    def lane_sum(values, total):
        for i in range(values.shape[1] // 128):
            total = total + values[:, i * 128:(i + 1) * 128]
        return total

    contract = (((1,), (1,)), ((), ()))

    def score_old(step, top):
        at = pl.multiple_of(step * key_block, key_block)
        held = held_ref[:, pl.ds(at, key_block)]
        held = jnp.where((held >= 0) & (held < start), held, HIDE)
        keys = ko_ref[pl.ds(at, key_block), :]
        for span in spans:
            values = lax.dot_general(query[span], keys, contract, preferred_element_type=jnp.float32)
            values = jnp.where(held > oldest[span], values * scale, -jnp.inf)
            score_ref[span, pl.ds(at, key_block)] = values
            peak_ref[span, :] = lane_max(values, peak_ref[span, :])
        return top

    def score_new(step, top):
        at = pl.multiple_of(step * new_block, new_block)
        fresh = at + lax.broadcasted_iota(jnp.int32, (1, new_block), 1)
        keys = kn_ref[pl.ds(at, new_block), :]
        for span in spans:
            values = lax.dot_general(query[span], keys, contract, preferred_element_type=jnp.float32)
            values = jnp.where(fresh <= token[span], values * scale, -jnp.inf)
            score_ref[span, pl.ds(pl.multiple_of(window + at, new_block), new_block)] = values
            peak_ref[span, :] = lane_max(values, peak_ref[span, :])
        return top

    old_steps = (jnp.minimum(start, window) + key_block - 1) // key_block
    new_steps = (block * rows + rows + new_block - 1) // new_block
    peak_ref[...] = jnp.full_like(peak_ref, -jnp.inf)
    lax.fori_loop(0, old_steps, score_old, 0)
    lax.fori_loop(0, new_steps, score_new, 0)
    top_ref[...] = jnp.max(peak_ref[...], axis=1, keepdims=True)
    total_ref[...] = jnp.zeros_like(total_ref)
    mixed_ref[...] = jnp.zeros_like(mixed_ref)

    def weigh(at, size, value_ref, value_at, carry):
        value = value_ref[pl.ds(value_at, size), :]
        for span in spans:
            weights = jnp.exp2(score_ref[span, pl.ds(at, size)] - top_ref[span, :])
            total_ref[span, :] = lane_sum(weights, total_ref[span, :])
            mixed_ref[span, :] += jnp.dot(weights.astype(jnp.bfloat16), value, preferred_element_type=jnp.float32)
        return carry

    def mix_old(step, carry):
        at = pl.multiple_of(step * key_block, key_block)
        return weigh(at, key_block, vo_ref, at, carry)

    def mix_new(step, carry):
        at = pl.multiple_of(step * new_block, new_block)
        return weigh(pl.multiple_of(window + at, new_block), new_block, vn_ref, at, carry)

    lax.fori_loop(0, old_steps, mix_old, 0)
    lax.fori_loop(0, new_steps, mix_new, 0)
    mixed = (mixed_ref[...] / jnp.sum(total_ref[...], axis=1, keepdims=True)).astype(jnp.bfloat16)
    here = pl.ds(pl.multiple_of(block * rows, rows), rows)
    for g in range(group):
        o_ref[:, g * head_dim:(g + 1) * head_dim] = mixed[g * rows:(g + 1) * rows]
        all_ref[here, g * head_dim:(g + 1) * head_dim] = mixed[g * rows:(g + 1) * rows]

    tiles, _, cols = tile_ref.shape

    def tile_copy(i):
        return pltpu.make_async_copy(weight_ref.at[layer, :, i * cols:(i + 1) * cols], tile_ref.at[i], tile_sem.at[i])

    def stage_copy(i):
        return pltpu.make_async_copy(stage_ref.at[:, i * cols:(i + 1) * cols], lead_ref.at[:, i * cols:(i + 1) * cols], stage_sem.at[i])

    @pl.when(block == 0)
    def _():
        for i in range(tiles):
            tile_copy(i).start()

    @pl.when(block == pl.num_programs(0) - 1)
    def _():
        shards = table_ref.shape[0] // 2
        part = all_ref.shape[0] // table_ref.shape[0]
        picked = [all_ref[pl.ds(pl.multiple_of(table_ref[shards + i] * part, part), part), :] for i in range(shards)]
        picked = jnp.concatenate(picked, axis=0)
        for i in range(tiles):
            tile_copy(i).wait()
            stage_ref[:, i * cols:(i + 1) * cols] = jnp.dot(picked, tile_ref[i], preferred_element_type=jnp.float32).astype(jnp.bfloat16)
            stage_copy(i).start()
        for i in range(tiles):
            stage_copy(i).wait()


def attend(query, key_new, value_new, key_cache, value_cache, held, start_pos, table, w_o, layer, seq, rows=256, key_block=2048, new_block=512):
    chunk, q_cols = query.shape
    window, head_dim = key_cache.shape[2:]
    group = q_cols // head_dim
    keys = window + chunk
    model = w_o.shape[2]
    cols = 1024
    whole = pl.BlockSpec((chunk, head_dim), lambda i, *_: (0, 0))
    cache = pl.BlockSpec((None, None, window, head_dim), lambda i, *_: (layer, seq, 0, 0))
    return pl.pallas_call(
        functools.partial(attention_kernel, layer=layer, seq=seq, group=group, key_block=key_block, new_block=new_block),
        grid_spec=pltpu.PrefetchScalarGridSpec(
            num_scalar_prefetch=2,
            grid=(chunk // rows,),
            in_specs=[pl.BlockSpec((rows, q_cols), lambda i, *_: (i, 0)), whole, whole, cache, cache, pl.BlockSpec((None, 1, window), lambda i, *_: (seq, 0, 0)), pl.BlockSpec(memory_space=pl.ANY)],
            out_specs=[pl.BlockSpec((rows, q_cols), lambda i, *_: (i, 0)), pl.BlockSpec(memory_space=pl.ANY)],
            scratch_shapes=[pltpu.VMEM((rows * group, keys), jnp.float32), pltpu.VMEM((rows * group, 128), jnp.float32), pltpu.VMEM((rows * group, 1), jnp.float32), pltpu.VMEM((rows * group, 128), jnp.float32), pltpu.VMEM((rows * group, head_dim), jnp.float32),
                pltpu.VMEM((chunk, q_cols), jnp.bfloat16), pltpu.VMEM((model // cols, q_cols, cols), jnp.bfloat16), pltpu.VMEM((chunk // 2, model), jnp.bfloat16),
                pltpu.SemaphoreType.DMA((model // cols,)), pltpu.SemaphoreType.DMA((model // cols,))],
        ),
        out_shape=[jax.ShapeDtypeStruct((chunk, q_cols), jnp.bfloat16), jax.ShapeDtypeStruct((chunk // 2, model), jnp.bfloat16)],
        compiler_params=pltpu.CompilerParams(dimension_semantics=('arbitrary',), vmem_limit_bytes=VMEM_LIMIT),
        cost_estimate=pl.CostEstimate(flops=8 * chunk * q_cols * keys, bytes_accessed=4 * (window + chunk) * head_dim + 4 * chunk * q_cols, transcendentals=0),
        name='attend',
    )(start_pos, table, query, key_new, value_new, key_cache, value_cache, held, w_o)


def stream_tile(weight_ref, ring_ref, sem_ref, step, steps, layer, first, ahead=0):
    slots, _, cols = ring_ref.shape

    def copy(at):
        slot = lax.rem(at, slots)
        columns = pl.ds(pl.multiple_of((first + at) * cols, cols), cols)
        return pltpu.make_async_copy(weight_ref.at[layer, :, columns], ring_ref.at[slot], sem_ref.at[slot])

    @pl.when(step == -ahead)
    def _():
        for i in range(min(slots - 1, steps)):
            copy(jnp.int32(i)).start()

    def take():
        @pl.when(step + slots - 1 < steps)
        def _():
            copy(step + slots - 1).start()

        copy(step).wait()
        return ring_ref[lax.rem(step, slots)]

    return take


def project_kernel(table_ref, *refs, shards, joined, layer, steps, first):
    acts_refs, (weight_ref, *refs), (ring_ref, sem_ref) = refs[:shards], refs[shards:-2], refs[-2:]
    weight = stream_tile(weight_ref, ring_ref, sem_ref, pl.program_id(0), steps, layer, first)()
    total = jnp.dot(jnp.concatenate([ref[...] for ref in acts_refs], axis=0), weight, preferred_element_type=jnp.float32)
    if not joined:
        refs[0][...] = total.astype(jnp.bfloat16)
    else:
        lead_ref, kept_ref, sent_ref = refs
        total = (total + lead_ref[...].astype(jnp.float32)).astype(jnp.bfloat16)
        kept_ref[...] = total[:total.shape[0] // 2]
        sent_ref[...] = total[total.shape[0] // 2:]


def project_rows(table, acts, part, weight, layer, lead, cols, slots=4, piece=0, pieces=1):
    depth, model = weight.shape[1:]
    shards = table.shape[0] // 2
    picked = acts.shape[0] // part == shards
    half = part * shards
    first = 0 if picked or lead is not None else shards
    model = model // pieces
    steps = model // cols
    out = lambda rows: pl.BlockSpec((rows, cols), lambda i, *_: (0, i))
    shape = lambda rows: jax.ShapeDtypeStruct((rows, model), jnp.bfloat16)
    shard = lambda at: pl.BlockSpec((part, depth), lambda i, places: (at if picked else places[at], 0))
    in_specs = [shard(first + k) for k in range(shards)] + [pl.BlockSpec(memory_space=pl.ANY)]
    args = [table] + [acts] * shards + [weight]
    if lead is None:
        out_specs, out_shape = [out(half)], [shape(half)]
    else:
        in_specs.append(pl.BlockSpec((half, cols), lambda i, *_: (0, piece * steps + i)))
        args.append(lead)
        out_specs, out_shape = [out(half // 2)] * 2, [shape(half // 2)] * 2
    return pl.pallas_call(
        functools.partial(project_kernel, shards=shards, joined=lead is not None, layer=layer, steps=steps, first=piece * steps),
        grid_spec=pltpu.PrefetchScalarGridSpec(
            num_scalar_prefetch=1,
            grid=(model // cols,),
            in_specs=in_specs,
            out_specs=out_specs,
            scratch_shapes=[pltpu.VMEM((slots, depth, cols), jnp.bfloat16), pltpu.SemaphoreType.DMA((slots,))],
        ),
        out_shape=out_shape,
        compiler_params=pltpu.CompilerParams(dimension_semantics=('arbitrary',), vmem_limit_bytes=VMEM_LIMIT),
        cost_estimate=pl.CostEstimate(flops=2 * half * depth * model, bytes_accessed=2 * (half * depth + depth * model + half * model), transcendentals=0),
        name='project_rows',
    )(*args)


def expand_kernel(table_ref, *refs, shards, layer, tiles):
    x_refs, (weight_ref, bias_ref, out_ref, ring_ref, sem_ref) = refs[:shards], refs[shards:]
    weight = stream_tile(weight_ref, ring_ref, sem_ref, pl.program_id(0), tiles, layer, 0)()
    acts = jnp.concatenate([ref[...] for ref in x_refs], axis=0)
    lifted = jnp.dot(acts, weight, preferred_element_type=jnp.float32) + bias_ref[...].astype(jnp.float32)
    out_ref[...] = jax.nn.gelu(lifted, approximate=True).astype(jnp.bfloat16)


def expand_rows(table, acts, weight, bias, layer, first, cols=256, slots=4):
    chunk, model = acts.shape
    width = weight.shape[2]
    tiles = width // cols
    shards = table.shape[0] // 2
    part = chunk // table.shape[0]
    rows = part * shards
    shard = lambda at: pl.BlockSpec((part, model), lambda i, places: (places[at], 0))
    return pl.pallas_call(
        functools.partial(expand_kernel, shards=shards, layer=layer, tiles=tiles),
        grid_spec=pltpu.PrefetchScalarGridSpec(
            num_scalar_prefetch=1,
            grid=(tiles,),
            in_specs=[shard(first + k) for k in range(shards)] + [pl.BlockSpec(memory_space=pl.ANY), pl.BlockSpec((None, 1, cols), lambda i, *_: (layer, 0, i))],
            out_specs=pl.BlockSpec((rows, cols), lambda i, *_: (0, i)),
            scratch_shapes=[pltpu.VMEM((slots, model, cols), jnp.bfloat16), pltpu.SemaphoreType.DMA((slots,))],
        ),
        out_shape=jax.ShapeDtypeStruct((rows, width), jnp.bfloat16),
        compiler_params=pltpu.CompilerParams(dimension_semantics=('arbitrary',), vmem_limit_bytes=VMEM_LIMIT),
        cost_estimate=pl.CostEstimate(flops=2 * rows * model * width, bytes_accessed=2 * (rows * model + model * width + rows * width), transcendentals=0),
        name='expand',
    )(table, *[acts] * shards, weight, bias)


def lead_kernel(table_ref, *refs, shards, layer, tiles, steps):
    x_refs, (up_ref, bias_ref, down_ref, out_ref, act_ref, up_ring, up_sem, down_ring, down_sem) = refs[:shards], refs[shards:]
    cols = up_ring.shape[2]
    step = pl.program_id(0)
    take_up = stream_tile(up_ref, up_ring, up_sem, step, tiles, layer, 0)
    take_down = stream_tile(down_ref, down_ring, down_sem, step - tiles, steps, layer, 0, ahead=2)

    @pl.when(step < tiles)
    def _():
        acts = jnp.concatenate([ref[...] for ref in x_refs], axis=0)
        at = pl.ds(pl.multiple_of(step * cols, cols), cols)
        lifted = jnp.dot(acts, take_up(), preferred_element_type=jnp.float32) + bias_ref[:, at].astype(jnp.float32)
        act_ref[:, at] = jax.nn.gelu(lifted, approximate=True).astype(jnp.bfloat16)

    @pl.when(step >= tiles)
    def _():
        out_ref[...] = jnp.dot(act_ref[...], take_down(), preferred_element_type=jnp.float32).astype(jnp.bfloat16)


def lead_rows(table, acts, w_up, bias, w_down, layer, up_cols=256, down_cols=512, slots=4):
    chunk, model = acts.shape
    width = w_up.shape[2]
    tiles, steps = width // up_cols, model // down_cols
    shards = table.shape[0] // 2
    part = chunk // table.shape[0]
    rows = part * shards
    shard = lambda at: pl.BlockSpec((part, model), lambda i, places: (places[at], 0))
    return pl.pallas_call(
        functools.partial(lead_kernel, shards=shards, layer=layer, tiles=tiles, steps=steps),
        grid_spec=pltpu.PrefetchScalarGridSpec(
            num_scalar_prefetch=1,
            grid=(tiles + steps,),
            in_specs=[shard(shards + k) for k in range(shards)] + [pl.BlockSpec(memory_space=pl.ANY), pl.BlockSpec((None, 1, width), lambda i, *_: (layer, 0, 0)), pl.BlockSpec(memory_space=pl.ANY)],
            out_specs=pl.BlockSpec((rows, down_cols), lambda i, *_: (0, jnp.maximum(i - tiles, 0))),
            scratch_shapes=[
                pltpu.VMEM((rows, width), jnp.bfloat16),
                pltpu.VMEM((slots, model, up_cols), jnp.bfloat16), pltpu.SemaphoreType.DMA((slots,)),
                pltpu.VMEM((slots, width, down_cols), jnp.bfloat16), pltpu.SemaphoreType.DMA((slots,)),
            ],
        ),
        out_shape=jax.ShapeDtypeStruct((rows, model), jnp.bfloat16),
        compiler_params=pltpu.CompilerParams(dimension_semantics=('arbitrary',), vmem_limit_bytes=VMEM_LIMIT),
        cost_estimate=pl.CostEstimate(flops=4 * rows * model * width, bytes_accessed=2 * (2 * rows * model + 2 * model * width), transcendentals=0),
        name='lead_rows',
    )(table, *[acts] * shards, w_up, bias, w_down)


def cache_kernel(start_ref, ko_ref, vo_ref, kn_ref, vn_ref, kout_ref, vout_ref, ring_ref):
    window, head_dim = ko_ref.shape
    chunk = kn_ref.shape[0]
    pad = 16
    span = chunk + pad
    first = lax.rem(start_ref[pl.program_id(1)], window)
    base = pl.multiple_of((first // pad) * pad, pad)
    inner = first - base
    line = lax.broadcasted_iota(jnp.int32, (span, head_dim), 0)
    for old_ref, new_ref, out_ref in ((ko_ref, kn_ref, kout_ref), (vo_ref, vn_ref, vout_ref)):
        ring_ref[0:window] = old_ref[...]
        ring_ref[window:window + span] = old_ref[0:span]
        fresh = jnp.concatenate([new_ref[...].astype(jnp.float32), jnp.zeros((pad, head_dim), jnp.float32)], axis=0)
        fresh = pltpu.roll(fresh, inner, 0)
        kept = ring_ref[pl.ds(base, span), :].astype(jnp.float32)
        mine = (line >= inner) & (line < inner + chunk)
        ring_ref[pl.ds(base, span), :] = jnp.where(mine, fresh, kept).astype(jnp.bfloat16)
        out_ref[span:window] = ring_ref[span:window]
        wrapped = ring_ref[window:window + span].astype(jnp.float32)
        plain = ring_ref[0:span].astype(jnp.float32)
        out_ref[0:span] = jnp.where(line < first + chunk - window, wrapped, plain).astype(jnp.bfloat16)


def update_caches(start_pos, key_cache, value_cache, key_new, value_new):
    layers, seqs, window, head_dim = key_cache.shape
    chunk = key_new.shape[2]
    old = pl.BlockSpec((None, None, window, head_dim), lambda i, j, *_: (i, j, 0, 0))
    new = pl.BlockSpec((None, None, chunk, head_dim), lambda i, j, *_: (i, j, 0, 0))
    return pl.pallas_call(
        cache_kernel,
        grid_spec=pltpu.PrefetchScalarGridSpec(
            num_scalar_prefetch=1,
            grid=(layers, seqs),
            in_specs=[old, old, new, new],
            out_specs=[old, old],
            scratch_shapes=[pltpu.VMEM((window + chunk + 16, head_dim), jnp.bfloat16)],
        ),
        out_shape=[jax.ShapeDtypeStruct(key_cache.shape, jnp.bfloat16)] * 2,
        compiler_params=pltpu.CompilerParams(dimension_semantics=('arbitrary', 'arbitrary'), vmem_limit_bytes=VMEM_LIMIT),
        cost_estimate=pl.CostEstimate(flops=1 << 24, bytes_accessed=8 * layers * seqs * window * head_dim, transcendentals=0),
        name='write_caches',
    )(start_pos, key_cache, value_cache, key_new, value_new)


def solution(mesh):
    row_spec = P('dp', 'tp', None)
    cache_spec = P(None, 'dp', None, 'tp', None)
    col_spec = P(None, None, 'tp')
    bias_spec = P(None, 'tp')
    in_specs = (row_spec, P('dp'), P('dp', None, None), P('dp', None, None), cache_spec, cache_spec, P('dp', None), P(), col_spec, bias_spec, col_spec, bias_spec, col_spec, bias_spec, P(None, 'tp', None), P(), col_spec, bias_spec, P(None, 'tp', None), P())
    out_specs = (row_spec, cache_spec, cache_spec, P('dp', None))
    count = mesh.shape['tp']
    first_axis = lambda core: 1 + core
    pairs_core = [(d, d ^ 1) for d in range(count)]
    pairs_first = [(d, ((d // 2) ^ first_axis(d % 2)) * 2 + d % 2) for d in range(count)]
    pairs_second = [(d, ((d // 2) ^ (3 - first_axis(d % 2))) * 2 + d % 2) for d in range(count)]

    def device_step(tokens, start_pos, cos_tab, sin_tab, key_cache, value_cache, slot_pos, norm_params, w_q, b_q, w_k, b_k, w_v, b_v, w_o, b_o, w_up, b_up, w_down, b_down):
        num_seqs, part, _ = tokens.shape
        chunk = cos_tab.shape[1]
        head_dim = cos_tab.shape[2]
        layers = key_cache.shape[0]
        window = key_cache.shape[2]
        keys_in = key_cache.reshape(layers, num_seqs, window, head_dim)
        values_in = value_cache.reshape(layers, num_seqs, window, head_dim)
        held = slot_pos[:, None, :]
        me = lax.axis_index('tp')
        chip, core = me // 2, me % 2
        near, far = 1 + core, 2 - core
        mine = [chip ^ flip for flip in (0, far, near, 3)]
        theirs = [chip ^ flip for flip in (0, near, far, 3)]
        order = [c * 2 + core for c in mine] + [c * 2 + 1 - core for c in theirs]
        table = jnp.stack(order).astype(jnp.int32)
        norms = norm_params
        out_bias = b_o[:, None, :]
        down_bias = b_down[:, None, :]
        latest = [None]
        turn = [0]

        def item(compute, *values):
            if latest[0] is not None:
                values = lax.optimization_barrier((*values, latest[0]))[:-1]
            results = compute(*values)
            latest[0] = results[0]
            return results

        def send(value, pairs):
            return lax.ppermute(value, 'tp', pairs)

        def gather(value):
            return lax.all_gather(value, 'tp', axis=0, tiled=True)

        up_bias = b_up[:, None, :]

        def add_came(kept, came):
            return ((kept[part:].astype(jnp.float32) + came[part:].astype(jnp.float32)).astype(jnp.bfloat16),)

        def scatter_sum(lead, acts, make_acts, weight, layer, cols):
            lead = send(lead, pairs_core)
            yield
            kept, sent = item(lambda acts: project_rows(table, make_acts(acts), part, weight, layer, lead, cols), acts)
            came = send(sent, pairs_first)
            yield
            onward, = item(add_came, kept, came)
            last = send(onward, pairs_second)
            yield
            return kept, came, last

        def scatter_last(lead, acts, layer, pieces=2):
            lead = send(lead, pairs_core)
            yield
            active = []
            state = []

            def make(acts, piece):
                if not active:
                    active.append(expand_rows(table, acts, w_up, up_bias, layer, 0))
                return project_rows(table, active[0], part, w_down, layer, lead, 512, 4, piece, pieces)

            for piece in range(pieces):
                kept, sent = item(functools.partial(make, piece=piece), acts)
                state.append((kept, send(sent, pairs_first)))
            yield
            lasts = []
            for kept, came in state:
                onward, = item(add_came, kept, came)
                lasts.append(send(onward, pairs_second))
            yield
            return [(kept, came, last) for (kept, came), last in zip(state, lasts)]

        def attention(gathered, layer, seq):
            query, key_new, value_new = qkv_project(gathered, cos_tab, sin_tab, w_q, w_k, w_v, b_q, b_k, b_v, layer, seq)
            fresh_keys[layer][seq] = key_new
            fresh_values[layer][seq] = value_new
            mixed, lead = attend(query, key_new, value_new, keys_in, values_in, held, start_pos, table, w_o, layer, seq)
            return lead, mixed

        def expand(gathered, layer):
            return lead_rows(table, gathered, w_up, up_bias, w_down, layer), gathered

        def finish(middle, *terms):
            sums = [kept[:part].astype(jnp.float32) + came[:part].astype(jnp.float32) + last.astype(jnp.float32) for kept, came, last in zip(*[iter(terms)] * 3)]
            summed = jnp.concatenate(sums, axis=1)
            return ((middle.astype(jnp.float32) + summed + b_down[layers - 1].astype(jnp.float32)).astype(jnp.bfloat16),)

        def join(base, *terms, bias, layer, which):
            middle, normed = normalize(base, seq_of[0], terms, (bias, layer), norms, layer + which // 4, which % 4)
            return normed, middle

        seq_of = [0]
        fresh_keys = [[None] * num_seqs for _ in range(layers)]
        fresh_values = [[None] * num_seqs for _ in range(layers)]
        hidden_out = [None] * num_seqs

        def stream(seq):
            base = tokens
            normed, = item(lambda: normalize(base, seq, None, None, norms, 0, 0))
            for layer in range(layers):
                gathered = gather(normed)
                yield
                lead, own = item(functools.partial(attention, layer=layer, seq=seq), gathered)
                terms = yield from scatter_sum(lead, own, lambda mixed: mixed, w_o, layer, 1024)
                seq_of[0] = seq
                normed, middle = item(lambda *terms: join(base, *terms, bias=out_bias, layer=layer, which=2), *terms)
                gathered = gather(normed)
                yield
                lead, own = item(functools.partial(expand, layer=layer), gathered)
                if layer + 1 == layers and seq == TURNS[-1]:
                    pieces = yield from scatter_last(lead, own, layer)
                    hidden_out[seq], = item(finish, middle, *[value for piece in pieces for value in piece])
                    break
                terms = yield from scatter_sum(lead, own, lambda acts: expand_rows(table, acts, w_up, up_bias, layer, 0), w_down, layer, 512)
                if layer + 1 < layers:
                    seq_of[0] = seq
                    normed, base = item(lambda *terms: join(middle, *terms, bias=down_bias, layer=layer, which=4), *terms)
                else:
                    hidden_out[seq], = item(finish, middle, *terms)
            yield

        streams = [stream(seq) for seq in range(num_seqs)]
        for step, seq in enumerate(TURNS):
            turn[0] = step
            next(streams[seq])
        fresh_keys = [jnp.stack(k) for k in fresh_keys]
        fresh_values = [jnp.stack(v) for v in fresh_values]
        key_out, value_out = update_caches(start_pos, keys_in, values_in, jnp.stack(fresh_keys), jnp.stack(fresh_values))
        first_slot = start_pos % window
        offset = (jnp.arange(window)[None, :] - first_slot[:, None]) % window
        pos_out = jnp.where(offset < chunk, start_pos[:, None] + offset, slot_pos)
        return jnp.stack(hidden_out), key_out.reshape(key_cache.shape), value_out.reshape(value_cache.shape), pos_out

    return jax.shard_map(device_step, mesh=mesh, in_specs=in_specs, out_specs=out_specs, check_vma=False)
```
